32 devices in a mesh: layer: 2 (over y), neuron: 4 (over z), token: 4 (over x, core).
Axes of the slice: x: 2, y: 2, z: 4, core: 2. Of those that a mesh axis runs over, the one named last changes fastest.
Arguments:
- tokens: bfloat16 [4096, 8192], P(('layer', 'token'), 'neuron'), parts along dimension 0, may hold values from -6 to 6
- up_weight: bfloat16 [16384, 14336], P(('layer', 'token'), 'neuron'), parts along dimension 0, may hold values from -0.0625 to 0.0625
- encoder: bfloat16 [16384, 1024], P(('layer', 'token'), 'neuron'), parts along dimension 0, may hold values from -0.0625 to 0.0625
- decoder: bfloat16 [2048, 14336], P(('layer', 'token'), 'neuron'), parts along dimension 0, may hold values from -0.1875 to 0.1875
Outputs:
- grad_encoder: float32 [16384, 1024], P(('layer', 'token'), 'neuron'), parts along dimension 0
- grad_decoder: float32 [2048, 14336], P(('layer', 'token'), 'neuron'), parts along dimension 0
The draws below stay inside these ranges and needn't reach their ends.
There are 2 independent parts, one for each index of `layer`. The reference program is written for one: setup_inputs(seed, part) draws one part's arguments, and reference() takes and returns one part's arrays. A program takes and returns all parts, laid end to end along the dimension named above; each array names one. Nothing has to cross between parts.
All inputs are finite; a program needn't handle non-finite values.
Results may differ from the reference program's by a relative error of at most 0.0034.
Values may be sent and summed in bfloat16 or wider, within the bound.
A program may use at most 128 MiB of HBM per device.

```python
import math
import jax
import jax.numpy as jnp

D = 8192
FF = 14336
RANK = 1024
TOKENS = 2048


def level_of(stream_key, shape, cuts, least, top_value):
    def one(axis_at, parts):
        steps = jax.random.uniform(jax.random.fold_in(jax.random.fold_in(stream_key, 6), axis_at), (parts,), jnp.float32, least / len(cuts), top_value / len(cuts))
        return jnp.repeat(jnp.exp(steps), shape[axis_at] // parts).reshape((-1,) + (1,) * (len(shape) - axis_at - 1))

    factor_of = one(*cuts[0])
    for cut in cuts[1:]:
        factor_of = factor_of * one(*cut)
    return factor_of


def noise(rng, dims, width, bound, shards=(), kind=jnp.bfloat16):
    loudness = level_of(rng, dims, shards, -0.22, 0.18) if shards else 1.0
    drawn = jax.random.normal(rng, dims, jnp.float32) * width * loudness
    return jnp.minimum(jnp.maximum(drawn, -bound), bound).astype(kind)


def setup_inputs(seed: int = 0, part: int = 0) -> dict:
    keys = jax.random.split(jax.random.key(seed), 5)
    own_keys = jax.random.split(jax.random.fold_in(keys[4], part), 5)
    return {
        "tokens": noise(own_keys[0], (TOKENS, D), 1.0, 6.0, ((0, 4), (1, 4))),
        "up_weight": noise(own_keys[1], (D, FF), D ** -0.5, 0.0625, ((0, 4), (1, 4))),
        "encoder": noise(own_keys[2], (D, RANK), D ** -0.5, 0.0625, ((0, 4), (1, 4))),
        "decoder": noise(own_keys[3], (RANK, FF), RANK ** -0.5, 0.1875, ((0, 4), (1, 4))),
    }


def reference(tokens, up_weight, encoder, decoder):
    labels = jax.nn.relu(jnp.dot(tokens, up_weight, preferred_element_type=jnp.float32))
    hidden = jnp.dot(tokens, encoder, preferred_element_type=jnp.float32).astype(jnp.bfloat16)
    predicted = jnp.dot(hidden, decoder, preferred_element_type=jnp.float32)
    scaled = ((predicted - labels) / math.sqrt(TOKENS)).astype(jnp.bfloat16)
    grad_decoder = jnp.dot(hidden.T, scaled, preferred_element_type=jnp.float32)
    back = jnp.dot(scaled, decoder.T, preferred_element_type=jnp.float32).astype(jnp.bfloat16)
    grad_encoder = jnp.dot(tokens.T, back, preferred_element_type=jnp.float32)
    return (grad_encoder, grad_decoder)
```

```python
import functools
import math

import jax
import jax.numpy as jnp
from jax import lax
from jax.experimental import pallas as pl
from jax.experimental.pallas import tpu as pltpu
from jax.sharding import PartitionSpec as P

CHUNKS = 4
COLUMN_PARTS = 2
PIECE_ROWS = 64
TILE = 256
VMEM_BYTES = 66 * 1000 * 1000


class Channel:
    def __init__(self, make):
        self.make = make

    def free(self, k):
        @pl.when(k >= 2)
        def _():
            for copy in self.make(k - 2):
                copy.wait_send()

    def start(self, k):
        for copy in self.make(k):
            copy.start()

    def take(self, k, which=None):
        copies = self.make(k)
        for i in range(len(copies)) if which is None else which:
            copies[i].wait_recv()

    def drain(self, count):
        for k in range(max(count - 2, 0), count):
            for copy in self.make(k):
                copy.wait_send()


def step_kernel(
    sizes, tok, up, enc, dec_in, out_e, out_d,
    w, e, tt, dec, hid, scaled, lab_s, lab_r, lab_o, lab_k, lx_s, lx_r,
    h_s, h_f, h_r, bo, b1_s, b1_r, b2_s, b2_r, b3_s, b3_r, bz, bk, ge, gd, acc,
    in_sem, tok_sem, first_sem, fwd_sem, dec_ss, dec_rs,
    l1_ss, l1_rs, l2_ss, l2_rs, h1_ss, h1_rs, h2_ss, h2_rs, h3_ss, h3_rs, h4_ss, h4_rs,
    b1_ss, b1_rs, b2_ss, b2_rs, b3_ss, b3_rs, b4_ss, b4_rs, gd_ss, gd_rs,
):
    chunks, g, width, cols, rank_part, rank_rows, depth, scale = sizes
    f32, bf16 = jnp.float32, jnp.bfloat16
    rows = 4 * g
    rank = dec.shape[0]
    t = lax.axis_index("token")
    z = lax.axis_index("neuron")
    x, c = t // 2, t % 2
    x2, c2 = 1 - x, 1 - c
    near = [t, 2 * x + c2, 2 * x2 + c, 2 * x2 + c2]
    quarter = [2 * c + x, 2 * c2 + x, 2 * c + x2, 2 * c2 + x2]

    def remote(src, dst, ssem, rsem, **where):
        return pltpu.make_async_remote_copy(
            src, dst, ssem, rsem, device_id=where, device_id_type=pl.DeviceIdType.MESH
        )

    def along(d):
        return (z + d) % depth

    def at(start, size, unit):
        return pl.ds(pl.multiple_of(start, unit), size)

    def group(i):
        return at(near[i] * g, g, g)

    def chunk_rows(k):
        return at(k * rows, rows, rows)

    def group_rows(k, i):
        return at(k * rows + near[i] * g, g, g)

    barrier = pltpu.get_barrier_semaphore()
    for i in range(1, 4):
        pl.semaphore_signal(
            barrier, inc=1, device_id={"token": near[i]}, device_id_type=pl.DeviceIdType.MESH
        )
    for d in range(1, depth):
        pl.semaphore_signal(
            barrier, inc=1, device_id={"neuron": along(d)}, device_id_type=pl.DeviceIdType.MESH
        )
    pl.semaphore_wait(barrier, 3 + depth - 1)

    def first_local(k):
        return pltpu.make_async_copy(
            tok.at[at(k * g, g, g), :], tt.at[group_rows(k, 0), :], tok_sem.at[k, t]
        )

    def first_remote(k):
        return remote(
            tok.at[at(k * g, g, g), :], tt.at[group_rows(k, 0), :],
            first_sem.at[k], tok_sem.at[k, t], token=z,
        )

    def first(lo, hi):
        @pl.when(t == z)
        def _():
            for k in range(lo, hi):
                first_local(k).start()

        @pl.when(t != z)
        def _():
            for k in range(lo, hi):
                first_remote(k).start()

    def decoder_copy(i):
        return remote(
            dec_in.at[:, at(quarter[i] * cols, cols, 128)],
            dec.at[at(t * rank_rows, rank_rows, rank_rows), :],
            dec_ss.at[i], dec_rs.at[i], token=near[i],
        )

    def decoder_wait(i):
        remote(
            dec_in.at[:, at(quarter[i] * cols, cols, 128)],
            dec.at[at(near[i] * rank_rows, rank_rows, rank_rows), :],
            dec_ss.at[i], dec_rs.at[i], token=near[i],
        ).wait_recv()

    decoder_own = pltpu.make_async_copy(
        dec_in.at[:, at(quarter[0] * cols, cols, 128)],
        dec.at[at(t * rank_rows, rank_rows, rank_rows), :],
        dec_rs.at[0],
    )
    load_e = pltpu.make_async_copy(enc, e, in_sem.at[0])
    load_w = pltpu.make_async_copy(up, w, in_sem.at[1])

    early = min(2, chunks)
    first(0, early)
    load_e.start()
    load_w.start()
    decoder_own.start()
    for i in (2, 3, 1):
        decoder_copy(i).start()
    first(early, chunks)
    ge[...] = jnp.zeros_like(ge)

    def piece(k, i):
        ref = tt.at[group_rows(k, i), :]
        sem = tok_sem.at[k, near[i]]
        up_copy = lambda: remote(
            ref, ref, fwd_sem.at[k % 2, i, 0], sem, neuron=jnp.minimum(z + 1, depth - 1)
        )
        down_copy = lambda: remote(
            ref, ref, fwd_sem.at[k % 2, i, 1], sem, neuron=jnp.maximum(z - 1, 0)
        )
        return up_copy, down_copy, (z >= t) & (z < depth - 1), (z <= t) & (z > 0)

    def forward(k, i):
        up_copy, down_copy, goes_up, goes_down = piece(k, i)
        if i == 0:
            @pl.when(t == z)
            def _():
                first_local(k).wait()

            @pl.when(t != z)
            def _():
                up_copy().wait_recv()
        else:
            up_copy().wait_recv()

        @pl.when((k >= 2) & goes_up)
        def _():
            up_copy().wait_send()

        @pl.when(goes_up)
        def _():
            up_copy().start()

        @pl.when((k >= 2) & goes_down)
        def _():
            down_copy().wait_send()

        @pl.when(goes_down)
        def _():
            down_copy().start()

    lab_core = Channel(lambda k: [
        remote(lab_s.at[k % 2], lab_r.at[k % 2], l1_ss.at[k % 2], l1_rs.at[k % 2], token=near[1])
    ])
    lab_x = Channel(lambda k: [
        remote(lx_s.at[k % 2], lx_r.at[k], l2_ss.at[k % 2], l2_rs.at[k], token=near[2])
    ])
    hid_sum = Channel(lambda k: [
        remote(h_s.at[k % 2, group(i), :], h_r.at[k % 2, i - 1],
               h1_ss.at[k % 2, i - 1], h1_rs.at[k % 2, i - 1], token=near[i])
        for i in range(1, 4)
    ])

    def hid_block(k, source):
        return hid.at[group_rows(k, 0), at(source * rank_part, rank_part, 128)]

    hid_z = Channel(lambda k: [
        remote(hid_block(k, z), hid_block(k, z),
               h2_ss.at[k % 2, d - 1], h2_rs.at[k % 2, d - 1], neuron=along(d))
        for d in range(1, depth)
    ])
    hid_xc = Channel(lambda k: [
        remote(hid.at[group_rows(k, 0), :], hid.at[group_rows(k, 0), :],
               h3_ss.at[k % 2, i - 1], h3_rs.at[k % 2, i - 1], token=near[i])
        for i in (1, 2)
    ])
    hid_relay = Channel(lambda k: [
        remote(hid.at[group_rows(k, 2), :], hid.at[group_rows(k, 2), :],
               h4_ss.at[k % 2], h4_rs.at[k % 2], token=near[1])
    ])
    back_core = Channel(lambda k: [
        remote(b1_s.at[k % 2], b1_r.at[k % 2], b1_ss.at[k % 2], b1_rs.at[k % 2], token=near[1])
    ])
    back_x = Channel(lambda k: [
        remote(b2_s.at[k % 2], b2_r.at[k % 2], b2_ss.at[k % 2], b2_rs.at[k % 2], token=near[2])
    ])
    back_z = Channel(lambda k: [
        remote(b3_s.at[k % 2, :, at(along(d) * rank_part, rank_part, 128)], b3_r.at[k % 2, d - 1],
               b3_ss.at[k % 2, d - 1], b3_rs.at[k % 2, d - 1], neuron=along(d))
        for d in range(1, depth)
    ])
    back_t = Channel(lambda k: [
        remote(bk.at[k % 2, group(0), :], bk.at[k % 2, group(0), :],
               b4_ss.at[k % 2, i - 1], b4_rs.at[k % 2, i - 1], token=near[i])
        for i in range(1, 4)
    ])

    def product(k):
        @pl.when(k == 0)
        def _():
            load_e.wait()

        hid_sum.free(k)
        part = jnp.dot(tt[chunk_rows(k), :], e[...], preferred_element_type=f32)
        h_f[...] = part
        h_s[k % 2] = part.astype(bf16)

        @pl.when(k == 0)
        def _():
            load_w.wait()

        lab_core.free(k)

        @pl.loop(0, 2 * cols // TILE)
        def _(n):
            at_w = at(c2 * 2 * cols + n * TILE, TILE, TILE)
            lab_s[k % 2, :, at(n * TILE, TILE, TILE)] = jnp.dot(
                tt[chunk_rows(k), :], w[:, at_w], preferred_element_type=f32
            ).astype(bf16)

        hid_sum.start(k)

        @pl.loop(0, 2 * cols // TILE)
        def _(n):
            @pl.when(n == 1)
            def _():
                lab_core.start(k)

            at_w = at(c * 2 * cols + n * TILE, TILE, TILE)
            lab_o[:, at(n * TILE, TILE, TILE)] = jnp.dot(
                tt[chunk_rows(k), :], w[:, at_w], preferred_element_type=f32
            )

        if 2 * cols // TILE < 2:
            lab_core.start(k)

    def label_core(k):
        lab_core.take(k)
        lab_x.free(k)
        there, here = at(x2 * cols, cols, 128), at(x * cols, cols, 128)
        lx_s[k % 2] = (lab_o[:, there] + lab_r[k % 2, :, there].astype(f32)).astype(bf16)
        lab_k[k % 2] = lab_o[:, here] + lab_r[k % 2, :, here].astype(f32)

    def hidden_sum(k):
        hid_sum.take(k)
        hid_z.free(k)
        total = h_f[group(0), :]
        for i in range(3):
            total = total + h_r[k % 2, i].astype(f32)
        hid_block(k, z)[...] = total.astype(bf16)

    def hidden_z(k):
        for d in range(1, depth):
            source = along(depth - d)
            remote(hid_block(k, source), hid_block(k, source),
                   h2_ss.at[k % 2, d - 1], h2_rs.at[k % 2, d - 1], neuron=along(d)).wait_recv()
        hid_xc.free(k)
        hid_xc.start(k)

    def hidden_relay(k):
        hid_xc.take(k, [1])
        hid_relay.free(k)
        hid_relay.start(k)

    def error(k):
        hid_xc.take(k, [0])
        hid_relay.take(k)

        @pl.when(k == 0)
        def _():
            decoder_own.wait()
            for i in range(1, 4):
                decoder_wait(i)

        lab_x.take(k)
        predicted = jnp.dot(hid[chunk_rows(k), :], dec[...], preferred_element_type=f32)
        labels = jnp.maximum(lab_k[k % 2] + lx_r[k].astype(f32), 0.0)
        scaled[chunk_rows(k), :] = ((predicted - labels) * scale).astype(bf16)

    def back_product(k):
        back_core.free(k)
        bo[...] = lax.dot_general(
            scaled[chunk_rows(k), :], dec[...], (((1,), (1,)), ((), ())),
            preferred_element_type=f32,
        )
        b1_s[k % 2, 0] = bo[group(1), :].astype(bf16)
        b1_s[k % 2, 1] = bo[group(3), :].astype(bf16)

    def back_core_sum(k):
        back_core.take(k)
        back_x.free(k)
        b2_s[k % 2] = (bo[group(2), :] + b1_r[k % 2, 1].astype(f32)).astype(bf16)
        bo[group(0), :] = bo[group(0), :] + b1_r[k % 2, 0].astype(f32)

    def back_x_sum(k):
        back_x.take(k)
        back_z.free(k)
        total = bo[group(0), :] + b2_r[k % 2].astype(f32)
        bo[group(0), :] = total
        b3_s[k % 2] = total.astype(bf16)
        bz[k % 2] = bo[group(0), at(z * rank_part, rank_part, 128)]

    def back_z_sum(k):
        back_z.take(k)
        back_t.free(k)
        total = bz[k % 2]
        for d in range(depth - 1):
            total = total + b3_r[k % 2, d].astype(f32)
        bk[k % 2, group(0), :] = total.astype(bf16)

    def encoder_grad(k):
        for i in range(1, 4):
            remote(bk.at[k % 2, group(i), :], bk.at[k % 2, group(i), :],
                   b4_ss.at[k % 2, i - 1], b4_rs.at[k % 2, i - 1], token=near[i]).wait_recv()
        ge[...] += lax.dot_general(
            bk[k % 2], tt[chunk_rows(k), :], (((0,), (0,)), ((), ())), preferred_element_type=f32
        )

    def far(j):
        fx, fc = 1 - j // 2, (j + j // 2) % 2
        xx = x + fx - 2 * x * fx
        cc = c + fc - 2 * c * fc
        return 2 * xx + cc

    mine = at(quarter[0] * cols, cols, 128)

    def grad_remote(j):
        return remote(gd.at[j], out_d.at[:, mine], gd_ss.at[j], gd_rs.at[j], token=far(j))

    grad_local = pltpu.make_async_copy(gd.at[3], out_d.at[:, mine], gd_ss.at[3])

    def decoder_grad():
        @pl.loop(0, 4)
        def _(j):
            acc[...] = jnp.zeros_like(acc)

            @pl.loop(0, chunks)
            def _(k):
                acc[...] += lax.dot_general(
                    hid[chunk_rows(k), at(far(j) * rank_rows, rank_rows, 128)],
                    scaled[chunk_rows(k), :], (((0,), (0,)), ((), ())), preferred_element_type=f32,
                )
            gd[j] = acc[...].astype(bf16)

            @pl.when(j < 3)
            def _():
                grad_remote(j).start()

            @pl.when(j == 3)
            def _():
                grad_local.start()

    def staged(s, lag, *stages):
        k = s - lag

        @pl.when((k >= 0) & (k < chunks))
        def _():
            for stage in stages:
                stage(k)

    @pl.loop(0, chunks + 4)
    def _(s):
        staged(s, 0, lambda k: forward(k, 0))
        staged(s, 2, hidden_z)
        staged(s, 1, label_core, hidden_sum, lab_x.start, hid_z.start)
        staged(s, 3, back_core_sum, back_x.start)
        staged(s, 0, lambda k: forward(k, 1))
        staged(s, 2, hidden_relay)
        staged(s, 4, back_z_sum, back_t.start)
        staged(s, 3, back_x_sum, back_z.start)
        staged(s, 0, lambda k: forward(k, 2))
        staged(s, 2, error)

        @pl.when(s == chunks + 1)
        def _():
            decoder_grad()

        staged(s, 2, back_product, back_core.start)
        staged(s, 4, encoder_grad)
        staged(s, 0, lambda k: forward(k, 3), product)

    finish = pltpu.make_async_copy(ge, out_e, in_sem.at[0])
    finish.start()

    @pl.when(t != z)
    def _():
        for k in range(chunks):
            first_remote(k).wait_send()

    for i in range(1, 4):
        decoder_copy(i).wait_send()
    for k in range(max(chunks - 2, 0), chunks):
        for i in range(4):
            up_copy, down_copy, goes_up, goes_down = piece(k, i)

            @pl.when(goes_up)
            def _():
                up_copy().wait_send()

            @pl.when(goes_down)
            def _():
                down_copy().wait_send()

    for channel in (lab_core, lab_x, hid_sum, hid_z, hid_xc, hid_relay,
                    back_core, back_x, back_z, back_t):
        channel.drain(chunks)
    for j in range(3):
        grad_remote(j).wait_send()
        source = [2, 3, 1][j]
        remote(gd.at[j], out_d.at[:, at(quarter[source] * cols, cols, 128)],
               gd_ss.at[j], gd_rs.at[j], token=near[source]).wait_recv()
    grad_local.wait()
    finish.wait()


def fused(tokens, up_weight, encoder, decoder):
    row_count, width = tokens.shape
    depth = lax.axis_size("neuron")
    block = up_weight.shape[0]
    cols = up_weight.shape[1] // 4
    rank_part = encoder.shape[1]
    rank_rows = decoder.shape[0]
    rank = rank_rows * 4
    g = min(PIECE_ROWS, row_count)
    chunks = row_count // g
    rows = 4 * g
    total = rows * chunks
    scale = 1.0 / math.sqrt(total)
    sizes = (chunks, g, width, cols, rank_part, rank_rows, depth, scale)
    f32, bf16 = jnp.float32, jnp.bfloat16
    vmem = pltpu.VMEM
    dma = pltpu.SemaphoreType.DMA
    scratch = [
        vmem((block, 4 * cols), bf16), vmem((block, rank_part), bf16), vmem((total, block), bf16),
        vmem((rank, cols), bf16), vmem((total, rank), bf16), vmem((total, cols), bf16),
        vmem((2, rows, 2 * cols), bf16), vmem((2, rows, 2 * cols), bf16),
        vmem((rows, 2 * cols), f32), vmem((2, rows, cols), f32),
        vmem((2, rows, cols), bf16), vmem((chunks, rows, cols), bf16),
        vmem((2, rows, rank_part), bf16), vmem((rows, rank_part), f32),
        vmem((2, 3, g, rank_part), bf16),
        vmem((rows, rank), f32), vmem((2, 2, g, rank), bf16), vmem((2, 2, g, rank), bf16),
        vmem((2, g, rank), bf16), vmem((2, g, rank), bf16),
        vmem((2, g, rank), bf16), vmem((2, depth - 1, g, rank_part), bf16),
        vmem((2, g, rank_part), f32), vmem((2, rows, rank_part), bf16),
        vmem((rank_part, block), f32), vmem((4, rank_rows, cols), bf16), vmem((rank_rows, cols), f32),
        dma((2,)), dma((chunks, 4)), dma((chunks,)), dma((2, 4, 2)), dma((4,)), dma((4,)),
        dma((2,)), dma((2,)), dma((2,)), dma((chunks,)),
        dma((2, 3)), dma((2, 3)), dma((2, depth - 1)), dma((2, depth - 1)),
        dma((2, 2)), dma((2, 2)), dma((2,)), dma((2,)),
        dma((2,)), dma((2,)), dma((2,)), dma((2,)),
        dma((2, depth - 1)), dma((2, depth - 1)), dma((2, 3)), dma((2, 3)), dma((4,)), dma((4,)),
    ]
    anywhere = pl.BlockSpec(memory_space=pl.ANY)
    grad_e, grad_d = pl.pallas_call(
        functools.partial(step_kernel, sizes),
        out_shape=(
            jax.ShapeDtypeStruct((rank_part, block), f32),
            jax.ShapeDtypeStruct((rank_rows, 4 * cols), bf16),
        ),
        in_specs=[anywhere] * 4,
        out_specs=(anywhere, anywhere),
        scratch_shapes=scratch,
        compiler_params=pltpu.CompilerParams(
            collective_id=0, has_side_effects=True, vmem_limit_bytes=VMEM_BYTES
        ),
        name="step",
    )(tokens, up_weight, encoder, decoder)
    return grad_e.T, grad_d.astype(f32)


def fits(mesh, tokens, up_weight, encoder, decoder):
    deep, wide = mesh.shape["neuron"], mesh.shape["token"]
    row_count = tokens.shape[0] // (mesh.shape["layer"] * wide)
    return (
        wide == 4
        and deep == wide
        and up_weight.shape[1] % (deep * wide * 128) == 0
        and up_weight.shape[1] % (deep * 2 * TILE) == 0
        and encoder.shape[1] % (deep * 128) == 0
        and row_count % PIECE_ROWS == 0
    )


def multiply(left, right):
    return jnp.dot(left, right, preferred_element_type=jnp.float32)


def contract_rows(left, right):
    return lax.dot_general(
        left, right, (((0,), (0,)), ((), ())), preferred_element_type=jnp.float32
    )


def swap(value, axis, offset):
    size = lax.axis_size(axis)
    return lax.ppermute(value, axis, [(i, i ^ offset) for i in range(size)])


def block_at(value, index, width, dim):
    return lax.dynamic_slice_in_dim(value, index * width, width, dim)


def after(value, *earlier):
    return lax.optimization_barrier((value, *earlier))[0]


def reduce_relative(terms_of, axis, wire, trace=None):
    size = lax.axis_size(axis)
    ks = list(range(size))
    held = None
    bit = 1
    while bit < size:
        kept = [k for k in ks if not k & bit]
        sent = [k for k in ks if k & bit]
        if held is None:
            outgoing = terms_of(sent).astype(wire)
            own = terms_of(kept) if trace is None else terms_of(kept, outgoing)
        else:
            outgoing = jnp.stack([held[ks.index(k)] for k in sent]).astype(wire)
            own = jnp.stack([held[ks.index(k)] for k in kept])
        if trace is not None:
            trace.append([outgoing, own])
        held = own + swap(outgoing, axis, bit).astype(jnp.float32)
        ks = kept
        bit *= 2
    if held is None:
        held = terms_of(ks)
    return held[0]


def gather_absolute(value, axis):
    size = lax.axis_size(axis)
    me = lax.axis_index(axis)
    held = value[None]
    order = [0]
    bit = size // 2
    while bit:
        held = jnp.concatenate([held, swap(held, axis, bit)])
        order = order + [k ^ bit for k in order]
        bit //= 2
    place = [order.index(k) for k in range(size)]
    relative = [held[p] for p in place]
    for level in range(size.bit_length() - 1):
        step = 1 << level
        flip = (me & step) != 0
        relative = [
            jnp.where(flip, relative[j ^ step], relative[j]) for j in range(size)
        ]
    return jnp.concatenate(relative)


def per_device(tokens, up_weight, encoder, decoder):
    token_size = lax.axis_size("token")
    neuron_size = lax.axis_size("neuron")
    t = lax.axis_index("token")
    n = lax.axis_index("neuron")
    row_count, width = tokens.shape
    rank_part = encoder.shape[1]
    rank = decoder.shape[0] * token_size
    rank_rows = decoder.shape[0]
    features = width * neuron_size // token_size
    blocks = neuron_size // token_size
    total_rows = row_count * token_size
    chunks = CHUNKS
    rows = row_count // chunks
    scale = 1.0 / math.sqrt(total_rows)

    gathered = [
        lax.all_gather(tokens[c * rows : (c + 1) * rows], "neuron", axis=0, tiled=False)
        for c in range(chunks)
    ]
    decoder_whole = gather_absolute(decoder, "token")

    hiddens, errors, all_pieces = [], [], []
    previous, gates = None, []
    for c in range(chunks):
        source = gathered[c] if previous is None else after(gathered[c], *gates[-1])
        grouped = source.reshape(token_size, blocks, rows, width)

        def features_for(k):
            mine = lax.dynamic_index_in_dim(grouped, t ^ k, 0, keepdims=False)
            return mine.transpose(1, 0, 2).reshape(rows, features)

        pieces = [features_for(0)] + [
            swap(features_for(k), "token", k) for k in range(1, token_size)
        ]
        if previous is not None:
            pieces[1] = after(pieces[1], *previous)

        def terms(ks, weight, earlier=None):
            left = jnp.concatenate([pieces[k] for k in ks])
            if earlier is not None:
                left = after(left, earlier)
            return multiply(left, weight).reshape(len(ks), rows, weight.shape[1])

        label_trace = []
        sums = reduce_relative(
            lambda ks, earlier=None: terms(ks, up_weight, earlier),
            "token",
            jnp.bfloat16,
            label_trace,
        )
        hidden_part = reduce_relative(
            lambda ks: terms(ks, encoder), "token", jnp.float32
        ).astype(jnp.bfloat16)
        others = jnp.stack(
            [hidden_part]
            + [swap(hidden_part, "neuron", m) for m in range(1, neuron_size)]
        )
        hidden = jnp.concatenate(
            [
                lax.dynamic_index_in_dim(others, n ^ j, 0, keepdims=False)
                for j in range(neuron_size)
            ],
            axis=1,
        )
        labels = jax.nn.relu(sums)
        predicted = multiply(hidden, decoder_whole)
        scaled = ((predicted - labels) * scale).astype(jnp.bfloat16)
        previous = label_trace[-1][:1] + errors[-1:]
        gates.append(label_trace[0])
        hiddens.append(hidden)
        errors.append(scaled)
        all_pieces.append(pieces)

    hidden = jnp.concatenate(hiddens)
    scaled = jnp.concatenate(errors)
    columns = scaled.shape[1] // COLUMN_PARTS
    relative = [block_at(hidden, t ^ k, rank_rows, 1) for k in range(token_size)]
    grads = []
    for p in range(COLUMN_PARTS):
        part = scaled[:, p * columns : (p + 1) * columns]

        def grad_terms(ks, part=part):
            left = jnp.concatenate([relative[k] for k in ks], axis=1)
            return contract_rows(left, part).reshape(len(ks), rank_rows, columns)

        grads.append(reduce_relative(grad_terms, "token", jnp.bfloat16))

    back_terms = lax.dot_general(
        scaled, decoder_whole, (((1,), (1,)), ((), ())), preferred_element_type=jnp.float32
    )
    back = block_at(back_terms, n, rank_part, 1)
    for m in range(1, neuron_size):
        outgoing = block_at(back_terms, n ^ m, rank_part, 1).astype(jnp.bfloat16)
        back = back + swap(outgoing, "neuron", m).astype(jnp.float32)
    back = back.astype(jnp.bfloat16)
    backs = [back] + [swap(back, "token", k) for k in range(1, token_size)]
    grad_encoder = contract_rows(
        jnp.concatenate([pieces[k] for k in range(token_size) for pieces in all_pieces]),
        jnp.concatenate(backs),
    )
    return (grad_encoder, jnp.concatenate(grads, axis=1))


def solution(mesh):
    spec = P(("layer", "token"), "neuron")

    def step(tokens, up_weight, encoder, decoder):
        local = fused if fits(mesh, tokens, up_weight, encoder, decoder) else per_device
        return jax.shard_map(
            local, mesh=mesh, in_specs=(spec,) * 4, out_specs=(spec, spec), check_vma=False
        )(tokens, up_weight, encoder, decoder)

    return step
```

```python
import functools
import math

import jax
import jax.numpy as jnp
from jax import lax
from jax.experimental import pallas as pl
from jax.experimental.pallas import tpu as pltpu
from jax.sharding import PartitionSpec as P

CHUNKS = 4
COLUMN_PARTS = 2
PIECE_ROWS = 64
TILE = 256
KEPT = 3
AHEAD = 3
SCHEDULE = (
    ("label_core", 2), ("hidden_relay", 4), (0, 0), ("product", 1), ("encoder_grad", 9),
    ("hidden_z", 3), ("back_x", 6), (1, 0), ("back_core", 5), ("error", 4), ("hidden_core", 1),
    ("hidden_x", 2), (2, 0), ("back_product", 4), (3, 0), ("back_z", 7),
)
VMEM_BYTES = 66 * 1000 * 1000


class Channel:
    def __init__(self, make):
        self.make = make

    def free(self, k):
        @pl.when(k >= 2)
        def _():
            for copy in self.make(k - 2):
                copy.wait_send()

    def start(self, k):
        for copy in self.make(k):
            copy.start()

    def take(self, k, which=None):
        copies = self.make(k)
        for i in range(len(copies)) if which is None else which:
            copies[i].wait_recv()

    def drain(self, count):
        for k in range(max(count - 2, 0), count):
            for copy in self.make(k):
                copy.wait_send()


def step_kernel(
    sizes, tok, up, enc, dec_in, out_e, out_d,
    w, e, tt, dec, hid, scaled, lab_s, lab_r, lab_o, lab_k, lx_s, lx_r,
    h_s, h_f, h_r, hx_s, hx_r, bo, b1_s, b1_r, b2_s, b2_r, b3_s, b3_r, bz, bk, ge, gd, acc,
    in_sem, tok_sem, first_sem, fwd_sem, dec_ss, dec_rs,
    l1_ss, l1_rs, l2_ss, l2_rs, h1_ss, h1_rs, hx_ss, hx_rs, h2_ss, h2_rs, h3_ss, h3_rs, h4_ss, h4_rs,
    b1_ss, b1_rs, b2_ss, b2_rs, b3_ss, b3_rs, b4_ss, b4_rs, gd_ss, gd_rs,
):
    chunks, g, width, cols, rank_part, rank_rows, depth, scale = sizes
    f32, bf16 = jnp.float32, jnp.bfloat16
    rows = 4 * g
    rank = dec.shape[0]
    t = lax.axis_index("token")
    z = lax.axis_index("neuron")
    x, c = t // 2, t % 2
    x2, c2 = 1 - x, 1 - c
    near = [t, 2 * x + c2, 2 * x2 + c, 2 * x2 + c2]
    quarter = [2 * c + x, 2 * c2 + x, 2 * c + x2, 2 * c2 + x2]

    def remote(src, dst, ssem, rsem, **where):
        return pltpu.make_async_remote_copy(
            src, dst, ssem, rsem, device_id=where, device_id_type=pl.DeviceIdType.MESH
        )

    def along(d):
        return (z + d) % depth

    def at(start, size, unit):
        return pl.ds(pl.multiple_of(start, unit), size)

    def group(i):
        return at(near[i] * g, g, g)

    def chunk_rows(k):
        return at(k * rows, rows, rows)

    def group_rows(k, i):
        return at(k * rows + near[i] * g, g, g)

    barrier = pltpu.get_barrier_semaphore()
    for i in range(1, 4):
        pl.semaphore_signal(
            barrier, inc=1, device_id={"token": near[i]}, device_id_type=pl.DeviceIdType.MESH
        )
    for d in range(1, depth):
        pl.semaphore_signal(
            barrier, inc=1, device_id={"neuron": along(d)}, device_id_type=pl.DeviceIdType.MESH
        )
    pl.semaphore_wait(barrier, 3 + depth - 1)

    def first_local(k):
        return pltpu.make_async_copy(
            tok.at[at(k * g, g, g), :], tt.at[group_rows(k, 0), :], tok_sem.at[k, t]
        )

    def first_remote(k):
        return remote(
            tok.at[at(k * g, g, g), :], tt.at[group_rows(k, 0), :],
            first_sem.at[k], tok_sem.at[k, t], token=z,
        )

    def first(k):
        @pl.when(t == z)
        def _():
            first_local(k).start()

        @pl.when(t != z)
        def _():
            first_remote(k).start()

    def decoder_copy(i):
        return remote(
            dec_in.at[:, at(quarter[i] * cols, cols, 128)],
            dec.at[at(t * rank_rows, rank_rows, rank_rows), :],
            dec_ss.at[i], dec_rs.at[i], token=near[i],
        )

    def decoder_wait(i):
        remote(
            dec_in.at[:, at(quarter[i] * cols, cols, 128)],
            dec.at[at(near[i] * rank_rows, rank_rows, rank_rows), :],
            dec_ss.at[i], dec_rs.at[i], token=near[i],
        ).wait_recv()

    decoder_own = pltpu.make_async_copy(
        dec_in.at[:, at(quarter[0] * cols, cols, 128)],
        dec.at[at(t * rank_rows, rank_rows, rank_rows), :],
        dec_rs.at[0],
    )
    load_e = pltpu.make_async_copy(enc, e, in_sem.at[0])
    load_w = pltpu.make_async_copy(up, w, in_sem.at[1])

    for k in range(min(2, AHEAD, chunks)):
        first(k)
    load_e.start()
    load_w.start()
    decoder_own.start()
    for i in (2, 3, 1):
        decoder_copy(i).start()
    for k in range(2, min(AHEAD, chunks)):
        first(k)
    ge[...] = jnp.zeros_like(ge)

    def piece(k, i):
        ref = tt.at[group_rows(k, i), :]
        sem = tok_sem.at[k, near[i]]
        up_copy = lambda: remote(
            ref, ref, fwd_sem.at[k % 2, i, 0], sem, neuron=jnp.minimum(z + 1, depth - 1)
        )
        down_copy = lambda: remote(
            ref, ref, fwd_sem.at[k % 2, i, 1], sem, neuron=jnp.maximum(z - 1, 0)
        )
        return up_copy, down_copy, (z >= t) & (z < depth - 1), (z <= t) & (z > 0)

    def forward(k, i):
        up_copy, down_copy, goes_up, goes_down = piece(k, i)
        if i == 0:
            @pl.when(t == z)
            def _():
                first_local(k).wait()

            @pl.when(t != z)
            def _():
                up_copy().wait_recv()
        else:
            up_copy().wait_recv()

        @pl.when((k >= 2) & goes_up)
        def _():
            up_copy().wait_send()

        @pl.when(goes_up)
        def _():
            up_copy().start()

        @pl.when((k >= 2) & goes_down)
        def _():
            down_copy().wait_send()

        @pl.when(goes_down)
        def _():
            down_copy().start()

    lab_core = Channel(lambda k: [
        remote(lab_s.at[k % 2], lab_r.at[k % 2], l1_ss.at[k % 2], l1_rs.at[k % 2], token=near[1])
    ])
    lab_x = Channel(lambda k: [
        remote(lx_s.at[k % 2], lx_r.at[k], l2_ss.at[k % 2], l2_rs.at[k], token=near[2])
    ])
    hid_core = Channel(lambda k: [
        remote(h_s.at[k % 2], h_r.at[k], h1_ss.at[k % 2], h1_rs.at[k], token=near[1])
    ])
    hid_x = Channel(lambda k: [
        remote(hx_s.at[k % 2], hx_r.at[k], hx_ss.at[k % 2], hx_rs.at[k], token=near[2])
    ])

    def hid_block(k, source):
        return hid.at[group_rows(k, 0), at(source * rank_part, rank_part, 128)]

    hid_z = Channel(lambda k: [
        remote(hid_block(k, z), hid_block(k, z),
               h2_ss.at[k % 2, d - 1], h2_rs.at[k, d - 1], neuron=along(d))
        for d in range(1, depth)
    ])
    hid_xc = Channel(lambda k: [
        remote(hid.at[group_rows(k, 0), :], hid.at[group_rows(k, 0), :],
               h3_ss.at[k % 2, i - 1], h3_rs.at[k, i - 1], token=near[i])
        for i in (1, 2)
    ])
    hid_relay = Channel(lambda k: [
        remote(hid.at[group_rows(k, 2), :], hid.at[group_rows(k, 2), :],
               h4_ss.at[k % 2], h4_rs.at[k], token=near[1])
    ])
    back_core = Channel(lambda k: [
        remote(b1_s.at[k % 2], b1_r.at[k], b1_ss.at[k % 2], b1_rs.at[k], token=near[1])
    ])
    back_x = Channel(lambda k: [
        remote(b2_s.at[k % 2], b2_r.at[k], b2_ss.at[k % 2], b2_rs.at[k], token=near[2])
    ])
    back_z = Channel(lambda k: [
        remote(b3_s.at[k % 2, :, at(along(d) * rank_part, rank_part, 128)], b3_r.at[k, d - 1],
               b3_ss.at[k % 2, d - 1], b3_rs.at[k, d - 1], neuron=along(d))
        for d in range(1, depth)
    ])
    back_t = Channel(lambda k: [
        remote(bk.at[k, group(0), :], bk.at[k, group(0), :],
               b4_ss.at[k % 2, i - 1], b4_rs.at[k, i - 1], token=near[i])
        for i in range(1, 4)
    ])

    def product(k):
        @pl.when(k == 0)
        def _():
            load_e.wait()

        hid_core.free(k)
        h_f[k % KEPT] = jnp.dot(tt[chunk_rows(k), :], e[...], preferred_element_type=f32)
        h_s[k % 2, 0] = h_f[k % KEPT, group(1), :]
        h_s[k % 2, 1] = h_f[k % KEPT, group(3), :]

        @pl.when(k == 0)
        def _():
            load_w.wait()

        lab_core.free(k)

        @pl.loop(0, 2 * cols // TILE)
        def _(n):
            at_w = at(c2 * 2 * cols + n * TILE, TILE, TILE)
            lab_s[k % 2, :, at(n * TILE, TILE, TILE)] = jnp.dot(
                tt[chunk_rows(k), :], w[:, at_w], preferred_element_type=f32
            ).astype(bf16)

        hid_core.start(k)

        @pl.loop(0, 2 * cols // TILE)
        def _(n):
            @pl.when(n == 1)
            def _():
                lab_core.start(k)

            at_w = at(c * 2 * cols + n * TILE, TILE, TILE)
            lab_o[:, at(n * TILE, TILE, TILE)] = jnp.dot(
                tt[chunk_rows(k), :], w[:, at_w], preferred_element_type=f32
            )

        if 2 * cols // TILE < 2:
            lab_core.start(k)

    def label_core(k):
        lab_core.take(k)
        lab_x.free(k)
        there, here = at(x2 * cols, cols, 128), at(x * cols, cols, 128)
        lx_s[k % 2] = (lab_o[:, there] + lab_r[k % 2, :, there].astype(f32)).astype(bf16)
        lab_k[k % KEPT] = lab_o[:, here] + lab_r[k % 2, :, here].astype(f32)

    def hidden_core(k):
        hid_core.take(k)
        hid_x.free(k)
        hx_s[k % 2] = h_f[k % KEPT, group(2), :] + h_r[k, 1]
        h_f[k % KEPT, group(0), :] = h_f[k % KEPT, group(0), :] + h_r[k, 0]

    def hidden_x(k):
        hid_x.take(k)
        hid_z.free(k)
        hid_block(k, z)[...] = (h_f[k % KEPT, group(0), :] + hx_r[k]).astype(bf16)

    def hidden_z(k):
        for d in range(1, depth):
            source = along(depth - d)
            remote(hid_block(k, source), hid_block(k, source),
                   h2_ss.at[k % 2, d - 1], h2_rs.at[k, d - 1], neuron=along(d)).wait_recv()
        hid_xc.free(k)
        hid_xc.start(k)

    def hidden_relay(k):
        hid_xc.take(k, [1])
        hid_relay.free(k)
        hid_relay.start(k)

    def error(k):
        hid_xc.take(k, [0])
        hid_relay.take(k)

        @pl.when(k == 0)
        def _():
            decoder_own.wait()
            for i in range(1, 4):
                decoder_wait(i)

        lab_x.take(k)
        predicted = jnp.dot(hid[chunk_rows(k), :], dec[...], preferred_element_type=f32)
        labels = jnp.maximum(lab_k[k % KEPT] + lx_r[k].astype(f32), 0.0)
        scaled[chunk_rows(k), :] = ((predicted - labels) * scale).astype(bf16)

    def back_product(k):
        back_core.free(k)
        bo[k % 2] = lax.dot_general(
            scaled[chunk_rows(k), :], dec[...], (((1,), (1,)), ((), ())),
            preferred_element_type=f32,
        )
        b1_s[k % 2, 0] = bo[k % 2, group(1), :].astype(bf16)
        b1_s[k % 2, 1] = bo[k % 2, group(3), :].astype(bf16)

    def back_core_sum(k):
        back_core.take(k)
        back_x.free(k)
        b2_s[k % 2] = (bo[k % 2, group(2), :] + b1_r[k, 1].astype(f32)).astype(bf16)
        bo[k % 2, group(0), :] = bo[k % 2, group(0), :] + b1_r[k, 0].astype(f32)

    def back_x_sum(k):
        back_x.take(k)
        back_z.free(k)
        total = bo[k % 2, group(0), :] + b2_r[k].astype(f32)
        bo[k % 2, group(0), :] = total
        b3_s[k % 2] = total.astype(bf16)
        bz[k % 4] = bo[k % 2, group(0), at(z * rank_part, rank_part, 128)]

    def back_z_sum(k):
        back_z.take(k)
        back_t.free(k)
        total = bz[k % 4]
        for d in range(depth - 1):
            total = total + b3_r[k, d].astype(f32)
        bk[k, group(0), :] = total.astype(bf16)

    def encoder_grad(k):
        for i in range(1, 4):
            remote(bk.at[k, group(i), :], bk.at[k, group(i), :],
                   b4_ss.at[k % 2, i - 1], b4_rs.at[k, i - 1], token=near[i]).wait_recv()
        ge[...] += lax.dot_general(
            bk[k], tt[chunk_rows(k), :], (((0,), (0,)), ((), ())), preferred_element_type=f32
        )

    def far(j):
        fx, fc = 1 - j // 2, (j + j // 2) % 2
        xx = x + fx - 2 * x * fx
        cc = c + fc - 2 * c * fc
        return 2 * xx + cc

    mine = at(quarter[0] * cols, cols, 128)

    def grad_remote(j):
        return remote(gd.at[j], out_d.at[:, mine], gd_ss.at[j], gd_rs.at[j], token=far(j))

    grad_local = pltpu.make_async_copy(gd.at[3], out_d.at[:, mine], gd_ss.at[3])

    def decoder_grad():
        @pl.loop(0, 4)
        def _(j):
            acc[...] = jnp.zeros_like(acc)

            @pl.loop(0, chunks)
            def _(k):
                acc[...] += lax.dot_general(
                    hid[chunk_rows(k), at(far(j) * rank_rows, rank_rows, 128)],
                    scaled[chunk_rows(k), :], (((0,), (0,)), ((), ())), preferred_element_type=f32,
                )
            gd[j] = acc[...].astype(bf16)

            @pl.when(j < 3)
            def _():
                grad_remote(j).start()

            @pl.when(j == 3)
            def _():
                grad_local.start()

    def staged(s, lag, *stages):
        k = s - lag

        @pl.when((k >= 0) & (k < chunks))
        def _():
            for stage in stages:
                stage(k)

    def error_last(k):
        error(k)

        @pl.when(k == chunks - 1)
        def _():
            decoder_grad()

    stages = {
        "product": (product,),
        "label_core": (label_core, lab_x.start),
        "hidden_core": (hidden_core, hid_x.start),
        "hidden_x": (hidden_x, hid_z.start),
        "hidden_z": (hidden_z,),
        "hidden_relay": (hidden_relay,),
        "error": (error_last,),
        "back_product": (back_product, back_core.start),
        "back_core": (back_core_sum, back_x.start),
        "back_x": (back_x_sum, back_z.start),
        "back_z": (back_z_sum, back_t.start),
        "encoder_grad": (encoder_grad,),
    }
    for i in range(4):
        stages[i] = (functools.partial(lambda i, k: forward(k, i), i),)

    @pl.loop(0, chunks + max(lag for _, lag in SCHEDULE))
    def _(s):
        staged(s, -AHEAD, first)
        for name, lag in SCHEDULE:
            staged(s, lag, *stages[name])

    finish = pltpu.make_async_copy(ge, out_e, in_sem.at[0])
    finish.start()

    @pl.when(t != z)
    def _():
        for k in range(chunks):
            first_remote(k).wait_send()

    for i in range(1, 4):
        decoder_copy(i).wait_send()
    for k in range(max(chunks - 2, 0), chunks):
        for i in range(4):
            up_copy, down_copy, goes_up, goes_down = piece(k, i)

            @pl.when(goes_up)
            def _():
                up_copy().wait_send()

            @pl.when(goes_down)
            def _():
                down_copy().wait_send()

    for channel in (lab_core, lab_x, hid_core, hid_x, hid_z, hid_xc, hid_relay,
                    back_core, back_x, back_z, back_t):
        channel.drain(chunks)
    for j in range(3):
        grad_remote(j).wait_send()
        source = [2, 3, 1][j]
        remote(gd.at[j], out_d.at[:, at(quarter[source] * cols, cols, 128)],
               gd_ss.at[j], gd_rs.at[j], token=near[source]).wait_recv()
    grad_local.wait()
    finish.wait()


def fused(tokens, up_weight, encoder, decoder):
    row_count, width = tokens.shape
    depth = lax.axis_size("neuron")
    block = up_weight.shape[0]
    cols = up_weight.shape[1] // 4
    rank_part = encoder.shape[1]
    rank_rows = decoder.shape[0]
    rank = rank_rows * 4
    g = min(PIECE_ROWS, row_count)
    chunks = row_count // g
    rows = 4 * g
    total = rows * chunks
    scale = 1.0 / math.sqrt(total)
    sizes = (chunks, g, width, cols, rank_part, rank_rows, depth, scale)
    f32, bf16 = jnp.float32, jnp.bfloat16
    vmem = pltpu.VMEM
    dma = pltpu.SemaphoreType.DMA
    scratch = [
        vmem((block, 4 * cols), bf16), vmem((block, rank_part), bf16), vmem((total, block), bf16),
        vmem((rank, cols), bf16), vmem((total, rank), bf16), vmem((total, cols), bf16),
        vmem((2, rows, 2 * cols), bf16), vmem((2, rows, 2 * cols), bf16),
        vmem((rows, 2 * cols), f32), vmem((KEPT, rows, cols), f32),
        vmem((2, rows, cols), bf16), vmem((chunks, rows, cols), bf16),
        vmem((2, 2, g, rank_part), f32), vmem((KEPT, rows, rank_part), f32),
        vmem((chunks, 2, g, rank_part), f32),
        vmem((2, g, rank_part), f32), vmem((chunks, g, rank_part), f32),
        vmem((2, rows, rank), f32), vmem((2, 2, g, rank), bf16), vmem((chunks, 2, g, rank), bf16),
        vmem((2, g, rank), bf16), vmem((chunks, g, rank), bf16),
        vmem((2, g, rank), bf16), vmem((chunks, depth - 1, g, rank_part), bf16),
        vmem((4, g, rank_part), f32), vmem((chunks, rows, rank_part), bf16),
        vmem((rank_part, block), f32), vmem((4, rank_rows, cols), bf16), vmem((rank_rows, cols), f32),
        dma((2,)), dma((chunks, 4)), dma((chunks,)), dma((2, 4, 2)), dma((4,)), dma((4,)),
        dma((2,)), dma((2,)), dma((2,)), dma((chunks,)),
        dma((2,)), dma((chunks,)), dma((2,)), dma((chunks,)),
        dma((2, depth - 1)), dma((chunks, depth - 1)),
        dma((2, 2)), dma((chunks, 2)), dma((2,)), dma((chunks,)),
        dma((2,)), dma((chunks,)), dma((2,)), dma((chunks,)),
        dma((2, depth - 1)), dma((chunks, depth - 1)), dma((2, 3)), dma((chunks, 3)),
        dma((4,)), dma((4,)),
    ]
    anywhere = pl.BlockSpec(memory_space=pl.ANY)
    grad_e, grad_d = pl.pallas_call(
        functools.partial(step_kernel, sizes),
        out_shape=(
            jax.ShapeDtypeStruct((rank_part, block), f32),
            jax.ShapeDtypeStruct((rank_rows, 4 * cols), bf16),
        ),
        in_specs=[anywhere] * 4,
        out_specs=(anywhere, anywhere),
        scratch_shapes=scratch,
        compiler_params=pltpu.CompilerParams(
            collective_id=0, has_side_effects=True, vmem_limit_bytes=VMEM_BYTES
        ),
        name="step",
    )(tokens, up_weight, encoder, decoder)
    return grad_e.T, grad_d.astype(f32)


def fits(mesh, tokens, up_weight, encoder, decoder):
    deep, wide = mesh.shape["neuron"], mesh.shape["token"]
    row_count = tokens.shape[0] // (mesh.shape["layer"] * wide)
    return (
        wide == 4
        and deep == wide
        and up_weight.shape[1] % (deep * wide * 128) == 0
        and up_weight.shape[1] % (deep * 2 * TILE) == 0
        and encoder.shape[1] % (deep * 128) == 0
        and row_count % PIECE_ROWS == 0
    )


def multiply(left, right):
    return jnp.dot(left, right, preferred_element_type=jnp.float32)


def contract_rows(left, right):
    return lax.dot_general(
        left, right, (((0,), (0,)), ((), ())), preferred_element_type=jnp.float32
    )


def swap(value, axis, offset):
    size = lax.axis_size(axis)
    return lax.ppermute(value, axis, [(i, i ^ offset) for i in range(size)])


def block_at(value, index, width, dim):
    return lax.dynamic_slice_in_dim(value, index * width, width, dim)


def after(value, *earlier):
    return lax.optimization_barrier((value, *earlier))[0]


def reduce_relative(terms_of, axis, wire, trace=None):
    size = lax.axis_size(axis)
    ks = list(range(size))
    held = None
    bit = 1
    while bit < size:
        kept = [k for k in ks if not k & bit]
        sent = [k for k in ks if k & bit]
        if held is None:
            outgoing = terms_of(sent).astype(wire)
            own = terms_of(kept) if trace is None else terms_of(kept, outgoing)
        else:
            outgoing = jnp.stack([held[ks.index(k)] for k in sent]).astype(wire)
            own = jnp.stack([held[ks.index(k)] for k in kept])
        if trace is not None:
            trace.append([outgoing, own])
        held = own + swap(outgoing, axis, bit).astype(jnp.float32)
        ks = kept
        bit *= 2
    if held is None:
        held = terms_of(ks)
    return held[0]


def gather_absolute(value, axis):
    size = lax.axis_size(axis)
    me = lax.axis_index(axis)
    held = value[None]
    order = [0]
    bit = size // 2
    while bit:
        held = jnp.concatenate([held, swap(held, axis, bit)])
        order = order + [k ^ bit for k in order]
        bit //= 2
    place = [order.index(k) for k in range(size)]
    relative = [held[p] for p in place]
    for level in range(size.bit_length() - 1):
        step = 1 << level
        flip = (me & step) != 0
        relative = [
            jnp.where(flip, relative[j ^ step], relative[j]) for j in range(size)
        ]
    return jnp.concatenate(relative)


def per_device(tokens, up_weight, encoder, decoder):
    token_size = lax.axis_size("token")
    neuron_size = lax.axis_size("neuron")
    t = lax.axis_index("token")
    n = lax.axis_index("neuron")
    row_count, width = tokens.shape
    rank_part = encoder.shape[1]
    rank = decoder.shape[0] * token_size
    rank_rows = decoder.shape[0]
    features = width * neuron_size // token_size
    blocks = neuron_size // token_size
    total_rows = row_count * token_size
    chunks = CHUNKS
    rows = row_count // chunks
    scale = 1.0 / math.sqrt(total_rows)

    gathered = [
        lax.all_gather(tokens[c * rows : (c + 1) * rows], "neuron", axis=0, tiled=False)
        for c in range(chunks)
    ]
    decoder_whole = gather_absolute(decoder, "token")

    hiddens, errors, all_pieces = [], [], []
    previous, gates = None, []
    for c in range(chunks):
        source = gathered[c] if previous is None else after(gathered[c], *gates[-1])
        grouped = source.reshape(token_size, blocks, rows, width)

        def features_for(k):
            mine = lax.dynamic_index_in_dim(grouped, t ^ k, 0, keepdims=False)
            return mine.transpose(1, 0, 2).reshape(rows, features)

        pieces = [features_for(0)] + [
            swap(features_for(k), "token", k) for k in range(1, token_size)
        ]
        if previous is not None:
            pieces[1] = after(pieces[1], *previous)

        def terms(ks, weight, earlier=None):
            left = jnp.concatenate([pieces[k] for k in ks])
            if earlier is not None:
                left = after(left, earlier)
            return multiply(left, weight).reshape(len(ks), rows, weight.shape[1])

        label_trace = []
        sums = reduce_relative(
            lambda ks, earlier=None: terms(ks, up_weight, earlier),
            "token",
            jnp.bfloat16,
            label_trace,
        )
        hidden_part = reduce_relative(
            lambda ks: terms(ks, encoder), "token", jnp.float32
        ).astype(jnp.bfloat16)
        others = jnp.stack(
            [hidden_part]
            + [swap(hidden_part, "neuron", m) for m in range(1, neuron_size)]
        )
        hidden = jnp.concatenate(
            [
                lax.dynamic_index_in_dim(others, n ^ j, 0, keepdims=False)
                for j in range(neuron_size)
            ],
            axis=1,
        )
        labels = jax.nn.relu(sums)
        predicted = multiply(hidden, decoder_whole)
        scaled = ((predicted - labels) * scale).astype(jnp.bfloat16)
        previous = label_trace[-1][:1] + errors[-1:]
        gates.append(label_trace[0])
        hiddens.append(hidden)
        errors.append(scaled)
        all_pieces.append(pieces)

    hidden = jnp.concatenate(hiddens)
    scaled = jnp.concatenate(errors)
    columns = scaled.shape[1] // COLUMN_PARTS
    relative = [block_at(hidden, t ^ k, rank_rows, 1) for k in range(token_size)]
    grads = []
    for p in range(COLUMN_PARTS):
        part = scaled[:, p * columns : (p + 1) * columns]

        def grad_terms(ks, part=part):
            left = jnp.concatenate([relative[k] for k in ks], axis=1)
            return contract_rows(left, part).reshape(len(ks), rank_rows, columns)

        grads.append(reduce_relative(grad_terms, "token", jnp.bfloat16))

    back_terms = lax.dot_general(
        scaled, decoder_whole, (((1,), (1,)), ((), ())), preferred_element_type=jnp.float32
    )
    back = block_at(back_terms, n, rank_part, 1)
    for m in range(1, neuron_size):
        outgoing = block_at(back_terms, n ^ m, rank_part, 1).astype(jnp.bfloat16)
        back = back + swap(outgoing, "neuron", m).astype(jnp.float32)
    back = back.astype(jnp.bfloat16)
    backs = [back] + [swap(back, "token", k) for k in range(1, token_size)]
    grad_encoder = contract_rows(
        jnp.concatenate([pieces[k] for k in range(token_size) for pieces in all_pieces]),
        jnp.concatenate(backs),
    )
    return (grad_encoder, jnp.concatenate(grads, axis=1))


def solution(mesh):
    spec = P(("layer", "token"), "neuron")

    def step(tokens, up_weight, encoder, decoder):
        local = fused if fits(mesh, tokens, up_weight, encoder, decoder) else per_device
        return jax.shard_map(
            local, mesh=mesh, in_specs=(spec,) * 4, out_specs=(spec, spec), check_vma=False
        )(tokens, up_weight, encoder, decoder)

    return step
```

```python
import functools
import math

import jax
import jax.numpy as jnp
from jax import lax
from jax.experimental import pallas as pl
from jax.experimental.pallas import tpu as pltpu
from jax.sharding import PartitionSpec as P

CHUNKS = 4
COLUMN_PARTS = 2
PIECE_ROWS = 64
TILE = 256
KEPT = 3
RING = 4
AHEAD = 3
SCHEDULE = (
    ("label_core", 2), ("back_core", 5), ("hidden_relay", 4), (0, 0), ("back_z", 8),
    ("product", 1), (1, 0), ("hidden_z", 3), ("hidden_x", 2), (2, 0), ("error", 4),
    ("encoder_grad", 11), ("hidden_core", 1), ("back_x", 6), ("back_product", 4), (3, 0),
    ("back_pair", 9),
)
VMEM_BYTES = 67_000_000


class Channel:
    def __init__(self, make):
        self.make = make

    def each(self, k, which, action):
        for copy, *conditions in self.make(k):
            if conditions[which] is None:
                action(copy)
            else:
                pl.when(conditions[which])(functools.partial(action, copy))

    def free(self, k):
        @pl.when(k >= 2)
        def _():
            self.each(k - 2, 0, lambda copy: copy.wait_send())

    def start(self, k):
        self.each(k, 0, lambda copy: copy.start())

    def take(self, k):
        self.each(k, 1, lambda copy: copy.wait_recv())

    def drain(self, count):
        for k in range(max(count - 2, 0), count):
            self.each(k, 0, lambda copy: copy.wait_send())


def step_kernel(
    sizes, tok, up, enc, dec_in, out_e, out_d,
    w, e, tt, dec, hid, scaled, lab_s, lab_r, lab_o, lab_k, lx_s, lx_r,
    h_s, h_f, h_r, hx_s, hx_r, bo, b1_s, b1_r, b2_s, b2_r, b3_s, b3_r, b4_s, b4_r, bz, bk, ge, gd, acc,
    in_sem, tok_sem, first_sem, fwd_sem, dec_ss, dec_rs,
    l1_ss, l1_rs, l2_ss, l2_rs, h1_ss, h1_rs, hx_ss, hx_rs, h2_ss, h2_rs, h3_ss, h3_rs,
    h4_ss, h4_rs, h5_ss, h5_rs,
    b1_ss, b1_rs, b2_ss, b2_rs, b3_ss, b3_rs, b4_ss, b4_rs, b5_ss, b5_rs, gd_ss, gd_rs,
):
    chunks, g, width, cols, rank_part, rank_rows, depth, scale = sizes
    f32, bf16 = jnp.float32, jnp.bfloat16
    rows = 4 * g
    rank = dec.shape[0]
    t = lax.axis_index("token")
    z = lax.axis_index("neuron")
    x, c = t // 2, t % 2
    x2, c2 = 1 - x, 1 - c
    near = [t, 2 * x + c2, 2 * x2 + c, 2 * x2 + c2]
    quarter = [2 * c + x, 2 * c2 + x, 2 * c + x2, 2 * c2 + x2]

    def remote(src, dst, ssem, rsem, **where):
        return pltpu.make_async_remote_copy(
            src, dst, ssem, rsem, device_id=where, device_id_type=pl.DeviceIdType.MESH
        )

    def along(d):
        return (z + d) % depth

    def at(start, size, unit):
        return pl.ds(pl.multiple_of(start, unit), size)

    half, other_half = at(c * 2 * g, 2 * g, 2 * g), at(c2 * 2 * g, 2 * g, 2 * g)

    def half_rows(k):
        return at(k * rows + c * 2 * g, 2 * g, 2 * g)

    def block(index):
        return at(index * rank_part, rank_part, 128)

    steps = [(2 * x - 1) * d for d in range(1, depth)]
    ahead = [jnp.clip(z + d, 0, depth - 1) for d in steps]
    behind = [jnp.clip(z - d, 0, depth - 1) for d in steps]
    has_ahead = [(z + d >= 0) & (z + d < depth) for d in steps]
    has_behind = [(z - d >= 0) & (z - d < depth) for d in steps]

    def chunk_rows(k):
        return at(k * rows, rows, rows)

    def group_rows(k, i):
        return at(k * rows + quarter[i] * g, g, g)

    barrier = pltpu.get_barrier_semaphore()
    for i in range(1, 4):
        pl.semaphore_signal(
            barrier, inc=1, device_id={"token": near[i]}, device_id_type=pl.DeviceIdType.MESH
        )
    for d in range(1, depth):
        pl.semaphore_signal(
            barrier, inc=1, device_id={"neuron": along(d)}, device_id_type=pl.DeviceIdType.MESH
        )
    pl.semaphore_wait(barrier, 3 + depth - 1)

    def first_local(k):
        return pltpu.make_async_copy(
            tok.at[at(k * g, g, g), :], tt.at[group_rows(k, 0), :], tok_sem.at[k, t]
        )

    def first_remote(k):
        return remote(
            tok.at[at(k * g, g, g), :], tt.at[group_rows(k, 0), :],
            first_sem.at[k], tok_sem.at[k, t], token=z,
        )

    def first(k):
        @pl.when(t == z)
        def _():
            first_local(k).start()

        @pl.when(t != z)
        def _():
            first_remote(k).start()

    def decoder_copy(i):
        return remote(
            dec_in.at[:, at(quarter[i] * cols, cols, 128)],
            dec.at[at(t * rank_rows, rank_rows, rank_rows), :],
            dec_ss.at[i], dec_rs.at[i], token=near[i],
        )

    def decoder_wait(i):
        remote(
            dec_in.at[:, at(quarter[i] * cols, cols, 128)],
            dec.at[at(near[i] * rank_rows, rank_rows, rank_rows), :],
            dec_ss.at[i], dec_rs.at[i], token=near[i],
        ).wait_recv()

    decoder_own = pltpu.make_async_copy(
        dec_in.at[:, at(quarter[0] * cols, cols, 128)],
        dec.at[at(t * rank_rows, rank_rows, rank_rows), :],
        dec_rs.at[0],
    )
    load_e = pltpu.make_async_copy(enc, e, in_sem.at[0])
    load_w = pltpu.make_async_copy(up, w, in_sem.at[1])

    for k in range(min(2, AHEAD, chunks)):
        first(k)
    load_e.start()
    load_w.start()
    decoder_own.start()
    for i in (2, 3, 1):
        decoder_copy(i).start()
    for k in range(2, min(AHEAD, chunks)):
        first(k)
    ge[...] = jnp.zeros_like(ge)

    def piece(k, i):
        ref = tt.at[group_rows(k, i), :]
        sem = tok_sem.at[k, near[i]]
        up_copy = lambda: remote(
            ref, ref, fwd_sem.at[k % 2, i, 0], sem, neuron=jnp.minimum(z + 1, depth - 1)
        )
        down_copy = lambda: remote(
            ref, ref, fwd_sem.at[k % 2, i, 1], sem, neuron=jnp.maximum(z - 1, 0)
        )
        return up_copy, down_copy, (z >= t) & (z < depth - 1), (z <= t) & (z > 0)

    def forward(k, i):
        up_copy, down_copy, goes_up, goes_down = piece(k, i)
        if i == 0:
            @pl.when(t == z)
            def _():
                first_local(k).wait()

            @pl.when(t != z)
            def _():
                up_copy().wait_recv()
        else:
            up_copy().wait_recv()

        @pl.when((k >= 2) & goes_up)
        def _():
            up_copy().wait_send()

        @pl.when(goes_up)
        def _():
            up_copy().start()

        @pl.when((k >= 2) & goes_down)
        def _():
            down_copy().wait_send()

        @pl.when(goes_down)
        def _():
            down_copy().start()

    def single(src, dst, ssem, rsem, i):
        return Channel(lambda k: [
            (remote(src(k), dst(k), ssem.at[k % 2], rsem.at[k], token=near[i]), None, None)
        ])

    lab_core = Channel(lambda k: [(
        remote(lab_s.at[k % 2], lab_r.at[k % 2], l1_ss.at[k % 2], l1_rs.at[k % 2], token=near[1]),
        None, None,
    )])
    lab_x = single(lambda k: lx_s.at[k % 2], lambda k: lx_r.at[k % RING], l2_ss, l2_rs, 2)
    hid_core = single(lambda k: h_s.at[k % 2], lambda k: h_r.at[k], h1_ss, h1_rs, 1)
    hid_x = single(lambda k: hx_s.at[k % 2], lambda k: hx_r.at[k], hx_ss, hx_rs, 2)

    def hid_block(k, source):
        return hid.at[half_rows(k), block(source)]

    def spread(ref, ssem, rsem, sends, receives, where, offset=0):
        return lambda k: [
            (remote(ref(k, i), ref(k, i), ssem.at[k % 2, i + offset], rsem.at[k, i + offset],
                    **where(i)), sends[i], receives[i])
            for i in range(depth - 1)
        ]

    hid_z = Channel(spread(
        lambda k, i: hid_block(k, z), h2_ss, h2_rs, has_ahead, has_behind,
        lambda i: {"neuron": ahead[i]},
    ))
    hid_back = Channel(spread(
        lambda k, i: hid_block(k, behind[i]), h3_ss, h3_rs, has_behind, has_ahead,
        lambda i: {"token": near[2]},
    ))
    to_partner = lambda i: {"token": near[1]}
    kept = spread(
        lambda k, i: hid_block(k, behind[i]), h4_ss, h4_rs, has_behind, has_behind, to_partner, 1
    )
    hid_kept = Channel(lambda k: kept(k) + [(
        remote(hid_block(k, z), hid_block(k, z), h4_ss.at[k % 2, 0], h4_rs.at[k, 0], token=near[1]),
        None, None,
    )])
    hid_relay = Channel(spread(
        lambda k, i: hid_block(k, ahead[i]), h5_ss, h5_rs, has_ahead, has_ahead, to_partner
    ))
    back_core = single(lambda k: b1_s.at[k % 2], lambda k: b1_r.at[k], b1_ss, b1_rs, 1)
    back_x = Channel(lambda k: [
        (remote(b2_s.at[k % 2, :, block(behind[i])], b2_r.at[k, :, block(behind[i])],
                b2_ss.at[k % 2, i], b2_rs.at[k, i], token=near[2]), has_behind[i], has_ahead[i])
        for i in range(depth - 1)
    ])
    back_z = Channel(lambda k: [
        (remote(b3_s.at[k % 2, i], b3_r.at[k, i], b3_ss.at[k % 2, i], b3_rs.at[k, i],
                neuron=ahead[i]), has_ahead[i], has_behind[i])
        for i in range(depth - 1)
    ])
    back_pair = single(lambda k: b4_s.at[k % 2], lambda k: b4_r.at[k], b4_ss, b4_rs, 2)
    back_t = single(lambda k: bk.at[k, half, :], lambda k: bk.at[k, half, :], b5_ss, b5_rs, 1)

    def product(k):
        @pl.when(k == 0)
        def _():
            load_e.wait()

        hid_core.free(k)
        h_f[...] = jnp.dot(tt[chunk_rows(k), :], e[...], preferred_element_type=f32)
        h_s[k % 2] = h_f[other_half, :]

        @pl.when(k == 0)
        def _():
            load_w.wait()

        lab_core.free(k)

        @pl.loop(0, 2 * cols // TILE)
        def _(n):
            at_w = at(c2 * 2 * cols + n * TILE, TILE, TILE)
            lab_s[k % 2, :, at(n * TILE, TILE, TILE)] = jnp.dot(
                tt[chunk_rows(k), :], w[:, at_w], preferred_element_type=f32
            ).astype(bf16)

        hid_core.start(k)

        @pl.loop(0, 2 * cols // TILE)
        def _(n):
            @pl.when(n == 1)
            def _():
                lab_core.start(k)

            at_w = at(c * 2 * cols + n * TILE, TILE, TILE)
            lab_o[:, at(n * TILE, TILE, TILE)] = jnp.dot(
                tt[chunk_rows(k), :], w[:, at_w], preferred_element_type=f32
            )

        if 2 * cols // TILE < 2:
            lab_core.start(k)

    def label_core(k):
        lab_core.take(k)
        lab_x.free(k)
        there, here = at(x2 * cols, cols, 128), at(x * cols, cols, 128)
        lx_s[k % 2] = (lab_o[:, there] + lab_r[k % 2, :, there].astype(f32)).astype(bf16)
        lab_k[k % KEPT] = lab_o[:, here] + lab_r[k % 2, :, here].astype(f32)

    def hidden_core(k):
        hid_core.take(k)
        hid_x.free(k)
        hx_s[k % 2] = h_f[half, :] + h_r[k]

    def hidden_x(k):
        hid_x.take(k)
        hid_z.free(k)
        hid_block(k, z)[...] = (hx_s[k % 2] + hx_r[k]).astype(bf16)

    def hidden_z(k):
        hid_z.take(k)
        hid_back.free(k)
        hid_kept.free(k)
        hid_back.start(k)
        hid_kept.start(k)

    def hidden_relay(k):
        hid_back.take(k)
        hid_relay.free(k)
        hid_relay.start(k)

    def error(k):
        hid_kept.take(k)
        hid_relay.take(k)

        @pl.when(k == 0)
        def _():
            decoder_own.wait()
            for i in range(1, 4):
                decoder_wait(i)

        lab_x.take(k)
        predicted = jnp.dot(hid[chunk_rows(k), :], dec[...], preferred_element_type=f32)
        labels = jnp.maximum(lab_k[k % KEPT] + lx_r[k % RING].astype(f32), 0.0)
        scaled[chunk_rows(k), :] = ((predicted - labels) * scale).astype(bf16)

    def back_product(k):
        back_core.free(k)
        bo[k % 2] = lax.dot_general(
            scaled[chunk_rows(k), :], dec[...], (((1,), (1,)), ((), ())),
            preferred_element_type=f32,
        )
        b1_s[k % 2] = bo[k % 2, other_half, :].astype(bf16)

    def back_core_sum(k):
        back_core.take(k)
        back_x.free(k)
        total = bo[k % 2, half, :] + b1_r[k].astype(f32)
        bo[k % 2, half, :] = total
        b2_s[k % 2] = total.astype(bf16)

    def back_x_sum(k):
        back_x.take(k)
        back_z.free(k)
        for i in range(depth - 1):
            @pl.when(has_ahead[i])
            def _():
                b3_s[k % 2, i] = (
                    bo[k % 2, half, block(ahead[i])] + b2_r[k, :, block(ahead[i])].astype(f32)
                ).astype(bf16)
        bz[k % 4] = bo[k % 2, half, block(z)]

    def back_z_sum(k):
        back_z.take(k)
        back_pair.free(k)
        for i in range(depth - 1):
            @pl.when(has_behind[i])
            def _():
                bz[k % 4] = bz[k % 4] + b3_r[k, i].astype(f32)
        b4_s[k % 2] = bz[k % 4].astype(bf16)

    def back_pair_sum(k):
        back_pair.take(k)
        back_t.free(k)
        bk[k, half, :] = (bz[k % 4] + b4_r[k].astype(f32)).astype(bf16)

    def encoder_grad(k):
        remote(bk.at[k, other_half, :], bk.at[k, other_half, :],
               b5_ss.at[k % 2], b5_rs.at[k], token=near[1]).wait_recv()
        ge[...] += lax.dot_general(
            bk[k], tt[chunk_rows(k), :], (((0,), (0,)), ((), ())), preferred_element_type=f32
        )

    def far(j):
        fx, fc = 1 - j // 2, (j + j // 2) % 2
        xx = x + fx - 2 * x * fx
        cc = c + fc - 2 * c * fc
        return 2 * xx + cc

    mine = at(quarter[0] * cols, cols, 128)

    def grad_remote(j):
        return remote(gd.at[j], out_d.at[:, mine], gd_ss.at[j], gd_rs.at[j], token=far(j))

    grad_local = pltpu.make_async_copy(gd.at[3], out_d.at[:, mine], gd_ss.at[3])

    def decoder_grad():
        @pl.loop(0, 4)
        def _(j):
            acc[...] = jnp.zeros_like(acc)

            @pl.loop(0, chunks)
            def _(k):
                acc[...] += lax.dot_general(
                    hid[chunk_rows(k), at(far(j) * rank_rows, rank_rows, 128)],
                    scaled[chunk_rows(k), :], (((0,), (0,)), ((), ())), preferred_element_type=f32,
                )
            gd[j] = acc[...].astype(bf16)

            @pl.when(j < 3)
            def _():
                grad_remote(j).start()

            @pl.when(j == 3)
            def _():
                grad_local.start()

    def staged(s, lag, *stages):
        k = s - lag

        @pl.when((k >= 0) & (k < chunks))
        def _():
            for stage in stages:
                stage(k)

    def error_last(k):
        error(k)

        @pl.when(k == chunks - 1)
        def _():
            decoder_grad()

    stages = {
        "product": (product,),
        "label_core": (label_core, lab_x.start),
        "hidden_core": (hidden_core, hid_x.start),
        "hidden_x": (hidden_x, hid_z.start),
        "hidden_z": (hidden_z,),
        "hidden_relay": (hidden_relay,),
        "error": (error_last,),
        "back_product": (back_product, back_core.start),
        "back_core": (back_core_sum, back_x.start),
        "back_x": (back_x_sum, back_z.start),
        "back_z": (back_z_sum, back_pair.start),
        "back_pair": (back_pair_sum, back_t.start),
        "encoder_grad": (encoder_grad,),
    }
    for i in range(4):
        stages[i] = (functools.partial(lambda i, k: forward(k, i), i),)

    @pl.loop(0, chunks + max(lag for _, lag in SCHEDULE))
    def _(s):
        staged(s, -AHEAD, first)
        for name, lag in SCHEDULE:
            staged(s, lag, *stages[name])

    finish = pltpu.make_async_copy(ge, out_e, in_sem.at[0])
    finish.start()

    @pl.when(t != z)
    def _():
        for k in range(chunks):
            first_remote(k).wait_send()

    for i in range(1, 4):
        decoder_copy(i).wait_send()
    for k in range(max(chunks - 2, 0), chunks):
        for i in range(4):
            up_copy, down_copy, goes_up, goes_down = piece(k, i)

            @pl.when(goes_up)
            def _():
                up_copy().wait_send()

            @pl.when(goes_down)
            def _():
                down_copy().wait_send()

    for channel in (lab_core, lab_x, hid_core, hid_x, hid_z, hid_back, hid_kept, hid_relay,
                    back_core, back_x, back_z, back_pair, back_t):
        channel.drain(chunks)
    for j in range(3):
        grad_remote(j).wait_send()
        source = [2, 3, 1][j]
        remote(gd.at[j], out_d.at[:, at(quarter[source] * cols, cols, 128)],
               gd_ss.at[j], gd_rs.at[j], token=near[source]).wait_recv()
    grad_local.wait()
    finish.wait()


def fused(tokens, up_weight, encoder, decoder):
    row_count, width = tokens.shape
    depth = lax.axis_size("neuron")
    block = up_weight.shape[0]
    cols = up_weight.shape[1] // 4
    rank_part = encoder.shape[1]
    rank_rows = decoder.shape[0]
    rank = rank_rows * 4
    g = min(PIECE_ROWS, row_count)
    chunks = row_count // g
    rows = 4 * g
    total = rows * chunks
    scale = 1.0 / math.sqrt(total)
    sizes = (chunks, g, width, cols, rank_part, rank_rows, depth, scale)
    f32, bf16 = jnp.float32, jnp.bfloat16
    vmem = pltpu.VMEM
    dma = pltpu.SemaphoreType.DMA
    scratch = [
        vmem((block, 4 * cols), bf16), vmem((block, rank_part), bf16), vmem((total, block), bf16),
        vmem((rank, cols), bf16), vmem((total, rank), bf16), vmem((total, cols), bf16),
        vmem((2, rows, 2 * cols), bf16), vmem((2, rows, 2 * cols), bf16),
        vmem((rows, 2 * cols), f32), vmem((KEPT, rows, cols), f32),
        vmem((2, rows, cols), bf16), vmem((RING, rows, cols), bf16),
        vmem((2, 2 * g, rank_part), f32), vmem((rows, rank_part), f32),
        vmem((chunks, 2 * g, rank_part), f32),
        vmem((2, 2 * g, rank_part), f32), vmem((chunks, 2 * g, rank_part), f32),
        vmem((2, rows, rank), f32), vmem((2, 2 * g, rank), bf16), vmem((chunks, 2 * g, rank), bf16),
        vmem((2, 2 * g, rank), bf16), vmem((chunks, 2 * g, rank), bf16),
        vmem((2, depth - 1, 2 * g, rank_part), bf16),
        vmem((chunks, depth - 1, 2 * g, rank_part), bf16),
        vmem((2, 2 * g, rank_part), bf16), vmem((chunks, 2 * g, rank_part), bf16),
        vmem((4, 2 * g, rank_part), f32), vmem((chunks, rows, rank_part), bf16),
        vmem((rank_part, block), f32), vmem((4, rank_rows, cols), bf16), vmem((rank_rows, cols), f32),
        dma((2,)), dma((chunks, 4)), dma((chunks,)), dma((2, 4, 2)), dma((4,)), dma((4,)),
        dma((2,)), dma((2,)), dma((2,)), dma((chunks,)),
        dma((2,)), dma((chunks,)), dma((2,)), dma((chunks,)),
        dma((2, depth - 1)), dma((chunks, depth - 1)), dma((2, depth - 1)), dma((chunks, depth - 1)),
        dma((2, depth)), dma((chunks, depth)), dma((2, depth - 1)), dma((chunks, depth - 1)),
        dma((2,)), dma((chunks,)), dma((2, depth - 1)), dma((chunks, depth - 1)),
        dma((2, depth - 1)), dma((chunks, depth - 1)), dma((2,)), dma((chunks,)),
        dma((2,)), dma((chunks,)), dma((4,)), dma((4,)),
    ]
    anywhere = pl.BlockSpec(memory_space=pl.ANY)
    grad_e, grad_d = pl.pallas_call(
        functools.partial(step_kernel, sizes),
        out_shape=(
            jax.ShapeDtypeStruct((rank_part, block), f32),
            jax.ShapeDtypeStruct((rank_rows, 4 * cols), bf16),
        ),
        in_specs=[anywhere] * 4,
        out_specs=(anywhere, anywhere),
        scratch_shapes=scratch,
        compiler_params=pltpu.CompilerParams(
            collective_id=0, has_side_effects=True, vmem_limit_bytes=VMEM_BYTES
        ),
        name="step",
    )(tokens, up_weight, encoder, decoder)
    return grad_e.T, grad_d.astype(f32)


def fits(mesh, tokens, up_weight, encoder, decoder):
    deep, wide = mesh.shape["neuron"], mesh.shape["token"]
    row_count = tokens.shape[0] // (mesh.shape["layer"] * wide)
    return (
        wide == 4
        and deep == wide
        and up_weight.shape[1] % (deep * wide * 128) == 0
        and up_weight.shape[1] % (deep * 2 * TILE) == 0
        and encoder.shape[1] % (deep * 128) == 0
        and row_count % PIECE_ROWS == 0
    )


def multiply(left, right):
    return jnp.dot(left, right, preferred_element_type=jnp.float32)


def contract_rows(left, right):
    return lax.dot_general(
        left, right, (((0,), (0,)), ((), ())), preferred_element_type=jnp.float32
    )


def swap(value, axis, offset):
    size = lax.axis_size(axis)
    return lax.ppermute(value, axis, [(i, i ^ offset) for i in range(size)])


def block_at(value, index, width, dim):
    return lax.dynamic_slice_in_dim(value, index * width, width, dim)


def after(value, *earlier):
    return lax.optimization_barrier((value, *earlier))[0]


def reduce_relative(terms_of, axis, wire, trace=None):
    size = lax.axis_size(axis)
    ks = list(range(size))
    held = None
    bit = 1
    while bit < size:
        kept = [k for k in ks if not k & bit]
        sent = [k for k in ks if k & bit]
        if held is None:
            outgoing = terms_of(sent).astype(wire)
            own = terms_of(kept) if trace is None else terms_of(kept, outgoing)
        else:
            outgoing = jnp.stack([held[ks.index(k)] for k in sent]).astype(wire)
            own = jnp.stack([held[ks.index(k)] for k in kept])
        if trace is not None:
            trace.append([outgoing, own])
        held = own + swap(outgoing, axis, bit).astype(jnp.float32)
        ks = kept
        bit *= 2
    if held is None:
        held = terms_of(ks)
    return held[0]


def gather_absolute(value, axis):
    size = lax.axis_size(axis)
    me = lax.axis_index(axis)
    held = value[None]
    order = [0]
    bit = size // 2
    while bit:
        held = jnp.concatenate([held, swap(held, axis, bit)])
        order = order + [k ^ bit for k in order]
        bit //= 2
    place = [order.index(k) for k in range(size)]
    relative = [held[p] for p in place]
    for level in range(size.bit_length() - 1):
        step = 1 << level
        flip = (me & step) != 0
        relative = [
            jnp.where(flip, relative[j ^ step], relative[j]) for j in range(size)
        ]
    return jnp.concatenate(relative)


def per_device(tokens, up_weight, encoder, decoder):
    token_size = lax.axis_size("token")
    neuron_size = lax.axis_size("neuron")
    t = lax.axis_index("token")
    n = lax.axis_index("neuron")
    row_count, width = tokens.shape
    rank_part = encoder.shape[1]
    rank = decoder.shape[0] * token_size
    rank_rows = decoder.shape[0]
    features = width * neuron_size // token_size
    blocks = neuron_size // token_size
    total_rows = row_count * token_size
    chunks = CHUNKS
    rows = row_count // chunks
    scale = 1.0 / math.sqrt(total_rows)

    gathered = [
        lax.all_gather(tokens[c * rows : (c + 1) * rows], "neuron", axis=0, tiled=False)
        for c in range(chunks)
    ]
    decoder_whole = gather_absolute(decoder, "token")

    hiddens, errors, all_pieces = [], [], []
    previous, gates = None, []
    for c in range(chunks):
        source = gathered[c] if previous is None else after(gathered[c], *gates[-1])
        grouped = source.reshape(token_size, blocks, rows, width)

        def features_for(k):
            mine = lax.dynamic_index_in_dim(grouped, t ^ k, 0, keepdims=False)
            return mine.transpose(1, 0, 2).reshape(rows, features)

        pieces = [features_for(0)] + [
            swap(features_for(k), "token", k) for k in range(1, token_size)
        ]
        if previous is not None:
            pieces[1] = after(pieces[1], *previous)

        def terms(ks, weight, earlier=None):
            left = jnp.concatenate([pieces[k] for k in ks])
            if earlier is not None:
                left = after(left, earlier)
            return multiply(left, weight).reshape(len(ks), rows, weight.shape[1])

        label_trace = []
        sums = reduce_relative(
            lambda ks, earlier=None: terms(ks, up_weight, earlier),
            "token",
            jnp.bfloat16,
            label_trace,
        )
        hidden_part = reduce_relative(
            lambda ks: terms(ks, encoder), "token", jnp.float32
        ).astype(jnp.bfloat16)
        others = jnp.stack(
            [hidden_part]
            + [swap(hidden_part, "neuron", m) for m in range(1, neuron_size)]
        )
        hidden = jnp.concatenate(
            [
                lax.dynamic_index_in_dim(others, n ^ j, 0, keepdims=False)
                for j in range(neuron_size)
            ],
            axis=1,
        )
        labels = jax.nn.relu(sums)
        predicted = multiply(hidden, decoder_whole)
        scaled = ((predicted - labels) * scale).astype(jnp.bfloat16)
        previous = label_trace[-1][:1] + errors[-1:]
        gates.append(label_trace[0])
        hiddens.append(hidden)
        errors.append(scaled)
        all_pieces.append(pieces)

    hidden = jnp.concatenate(hiddens)
    scaled = jnp.concatenate(errors)
    columns = scaled.shape[1] // COLUMN_PARTS
    relative = [block_at(hidden, t ^ k, rank_rows, 1) for k in range(token_size)]
    grads = []
    for p in range(COLUMN_PARTS):
        part = scaled[:, p * columns : (p + 1) * columns]

        def grad_terms(ks, part=part):
            left = jnp.concatenate([relative[k] for k in ks], axis=1)
            return contract_rows(left, part).reshape(len(ks), rank_rows, columns)

        grads.append(reduce_relative(grad_terms, "token", jnp.bfloat16))

    back_terms = lax.dot_general(
        scaled, decoder_whole, (((1,), (1,)), ((), ())), preferred_element_type=jnp.float32
    )
    back = block_at(back_terms, n, rank_part, 1)
    for m in range(1, neuron_size):
        outgoing = block_at(back_terms, n ^ m, rank_part, 1).astype(jnp.bfloat16)
        back = back + swap(outgoing, "neuron", m).astype(jnp.float32)
    back = back.astype(jnp.bfloat16)
    backs = [back] + [swap(back, "token", k) for k in range(1, token_size)]
    grad_encoder = contract_rows(
        jnp.concatenate([pieces[k] for k in range(token_size) for pieces in all_pieces]),
        jnp.concatenate(backs),
    )
    return (grad_encoder, jnp.concatenate(grads, axis=1))


def solution(mesh):
    spec = P(("layer", "token"), "neuron")

    def step(tokens, up_weight, encoder, decoder):
        local = fused if fits(mesh, tokens, up_weight, encoder, decoder) else per_device
        return jax.shard_map(
            local, mesh=mesh, in_specs=(spec,) * 4, out_specs=(spec, spec), check_vma=False
        )(tokens, up_weight, encoder, decoder)

    return step
```

```python
import functools
import math

import jax
import jax.numpy as jnp
from jax import lax
from jax.experimental import pallas as pl
from jax.experimental.pallas import tpu as pltpu
from jax.sharding import PartitionSpec as P

CHUNKS = 4
COLUMN_PARTS = 2
PIECE_ROWS = 64
TILE = 256
KEPT = 3
RING = 4
AHEAD = 2
SCHEDULE = (
    ("label_core", 2), ("back_core", 5), ("hidden_relay", 4), (0, 0), ("product", 1), (1, 0),
    ("back_z", 8), ("hidden_x", 2), ("error", 4), ("hidden_z", 3), ("back_x", 6),
    ("encoder_grad", 11), ("back_product", 4), (2, 0), ("back_pair", 9), ("hidden_core", 1), (3, 0),
)
VMEM_BYTES = 67_000_000


class Channel:
    def __init__(self, make):
        self.make = make

    def each(self, k, which, action):
        for copy, *conditions in self.make(k):
            if conditions[which] is None:
                action(copy)
            else:
                pl.when(conditions[which])(functools.partial(action, copy))

    def free(self, k):
        @pl.when(k >= 2)
        def _():
            self.each(k - 2, 0, lambda copy: copy.wait_send())

    def start(self, k):
        self.each(k, 0, lambda copy: copy.start())

    def take(self, k):
        self.each(k, 1, lambda copy: copy.wait_recv())

    def drain(self, count):
        for k in range(max(count - 2, 0), count):
            self.each(k, 0, lambda copy: copy.wait_send())


def step_kernel(
    sizes, tok, up, enc, dec_in, out_e, out_d,
    w, e, tt, dec, hid, scaled, lab_s, lab_r, lab_o, lab_k, lx_s, lx_r,
    h_s, h_f, h_r, hx_s, hx_r, bo, b1_s, b1_r, b2_s, b2_r, b3_s, b3_r, b4_s, b4_r, bz, bk, ge, gd, acc,
    in_sem, tok_sem, first_sem, fwd_sem, dec_ss, dec_rs,
    l1_ss, l1_rs, l2_ss, l2_rs, h1_ss, h1_rs, hx_ss, hx_rs, h2_ss, h2_rs, h3_ss, h3_rs,
    h4_ss, h4_rs, h5_ss, h5_rs,
    b1_ss, b1_rs, b2_ss, b2_rs, b3_ss, b3_rs, b4_ss, b4_rs, b5_ss, b5_rs, gd_ss, gd_rs,
):
    chunks, g, width, cols, rank_part, rank_rows, depth, scale = sizes
    f32, bf16 = jnp.float32, jnp.bfloat16
    rows = 4 * g
    rank = dec.shape[0]
    t = lax.axis_index("token")
    z = lax.axis_index("neuron")
    x, c = t // 2, t % 2
    x2, c2 = 1 - x, 1 - c
    near = [t, 2 * x + c2, 2 * x2 + c, 2 * x2 + c2]
    quarter = [2 * c + x, 2 * c2 + x, 2 * c + x2, 2 * c2 + x2]

    def remote(src, dst, ssem, rsem, **where):
        return pltpu.make_async_remote_copy(
            src, dst, ssem, rsem, device_id=where, device_id_type=pl.DeviceIdType.MESH
        )

    def along(d):
        return (z + d) % depth

    def at(start, size, unit):
        return pl.ds(pl.multiple_of(start, unit), size)

    half, other_half = at(c * 2 * g, 2 * g, 2 * g), at(c2 * 2 * g, 2 * g, 2 * g)

    def half_rows(k):
        return at(k * rows + c * 2 * g, 2 * g, 2 * g)

    def block(index):
        return at(index * rank_part, rank_part, 128)

    steps = [(2 * x - 1) * d for d in range(1, depth)]
    ahead = [jnp.clip(z + d, 0, depth - 1) for d in steps]
    behind = [jnp.clip(z - d, 0, depth - 1) for d in steps]
    has_ahead = [(z + d >= 0) & (z + d < depth) for d in steps]
    has_behind = [(z - d >= 0) & (z - d < depth) for d in steps]

    def chunk_rows(k):
        return at(k * rows, rows, rows)

    def group_rows(k, i):
        return at(k * rows + quarter[i] * g, g, g)

    barrier = pltpu.get_barrier_semaphore()
    for i in range(1, 4):
        pl.semaphore_signal(
            barrier, inc=1, device_id={"token": near[i]}, device_id_type=pl.DeviceIdType.MESH
        )
    for d in range(1, depth):
        pl.semaphore_signal(
            barrier, inc=1, device_id={"neuron": along(d)}, device_id_type=pl.DeviceIdType.MESH
        )
    pl.semaphore_wait(barrier, 3 + depth - 1)

    def first_local(k):
        return pltpu.make_async_copy(
            tok.at[at(k * g, g, g), :], tt.at[group_rows(k, 0), :], tok_sem.at[k, t]
        )

    def first_remote(k):
        return remote(
            tok.at[at(k * g, g, g), :], tt.at[group_rows(k, 0), :],
            first_sem.at[k], tok_sem.at[k, t], token=z,
        )

    def first(k):
        @pl.when(t == z)
        def _():
            first_local(k).start()

        @pl.when(t != z)
        def _():
            first_remote(k).start()

    def decoder_copy(i):
        return remote(
            dec_in.at[:, at(quarter[i] * cols, cols, 128)],
            dec.at[at(t * rank_rows, rank_rows, rank_rows), :],
            dec_ss.at[i], dec_rs.at[i], token=near[i],
        )

    def decoder_wait(i):
        remote(
            dec_in.at[:, at(quarter[i] * cols, cols, 128)],
            dec.at[at(near[i] * rank_rows, rank_rows, rank_rows), :],
            dec_ss.at[i], dec_rs.at[i], token=near[i],
        ).wait_recv()

    decoder_own = pltpu.make_async_copy(
        dec_in.at[:, at(quarter[0] * cols, cols, 128)],
        dec.at[at(t * rank_rows, rank_rows, rank_rows), :],
        dec_rs.at[0],
    )
    load_e = pltpu.make_async_copy(enc, e, in_sem.at[0])
    load_w = pltpu.make_async_copy(up, w, in_sem.at[1])

    for k in range(min(2, AHEAD, chunks)):
        first(k)
    load_e.start()
    load_w.start()
    decoder_own.start()
    for i in (2, 3, 1):
        decoder_copy(i).start()
    for k in range(2, min(AHEAD, chunks)):
        first(k)
    ge[...] = jnp.zeros_like(ge)

    def piece(k, i):
        ref = tt.at[group_rows(k, i), :]
        sem = tok_sem.at[k, near[i]]
        up_copy = lambda: remote(
            ref, ref, fwd_sem.at[k % 2, i, 0], sem, neuron=jnp.minimum(z + 1, depth - 1)
        )
        down_copy = lambda: remote(
            ref, ref, fwd_sem.at[k % 2, i, 1], sem, neuron=jnp.maximum(z - 1, 0)
        )
        return up_copy, down_copy, (z >= t) & (z < depth - 1), (z <= t) & (z > 0)

    def forward(k, i):
        up_copy, down_copy, goes_up, goes_down = piece(k, i)
        if i == 0:
            @pl.when(t == z)
            def _():
                first_local(k).wait()

            @pl.when(t != z)
            def _():
                up_copy().wait_recv()
        else:
            up_copy().wait_recv()

        @pl.when((k >= 2) & goes_up)
        def _():
            up_copy().wait_send()

        @pl.when(goes_up)
        def _():
            up_copy().start()

        @pl.when((k >= 2) & goes_down)
        def _():
            down_copy().wait_send()

        @pl.when(goes_down)
        def _():
            down_copy().start()

    def single(src, dst, ssem, rsem, i):
        return Channel(lambda k: [
            (remote(src(k), dst(k), ssem.at[k % 2], rsem.at[k], token=near[i]), None, None)
        ])

    lab_core = Channel(lambda k: [(
        remote(lab_s.at[k % 2], lab_r.at[k % 2], l1_ss.at[k % 2], l1_rs.at[k % 2], token=near[1]),
        None, None,
    )])
    lab_x = single(lambda k: lx_s.at[k % 2], lambda k: lx_r.at[k % RING], l2_ss, l2_rs, 2)
    hid_core = single(lambda k: h_s.at[k % 2], lambda k: h_r.at[k], h1_ss, h1_rs, 1)
    hid_x = single(lambda k: hx_s.at[k % 2], lambda k: hx_r.at[k], hx_ss, hx_rs, 2)

    def hid_block(k, source):
        return hid.at[half_rows(k), block(source)]

    def spread(ref, ssem, rsem, sends, receives, where, offset=0):
        return lambda k: [
            (remote(ref(k, i), ref(k, i), ssem.at[k % 2, i + offset], rsem.at[k, i + offset],
                    **where(i)), sends[i], receives[i])
            for i in range(depth - 1)
        ]

    hid_z = Channel(spread(
        lambda k, i: hid_block(k, z), h2_ss, h2_rs, has_ahead, has_behind,
        lambda i: {"neuron": ahead[i]},
    ))
    hid_back = Channel(spread(
        lambda k, i: hid_block(k, behind[i]), h3_ss, h3_rs, has_behind, has_ahead,
        lambda i: {"token": near[2]},
    ))
    to_partner = lambda i: {"token": near[1]}
    kept = spread(
        lambda k, i: hid_block(k, behind[i]), h4_ss, h4_rs, has_behind, has_behind, to_partner, 1
    )
    hid_kept = Channel(lambda k: kept(k) + [(
        remote(hid_block(k, z), hid_block(k, z), h4_ss.at[k % 2, 0], h4_rs.at[k, 0], token=near[1]),
        None, None,
    )])
    hid_relay = Channel(spread(
        lambda k, i: hid_block(k, ahead[i]), h5_ss, h5_rs, has_ahead, has_ahead, to_partner
    ))
    back_core = single(lambda k: b1_s.at[k % 2], lambda k: b1_r.at[k], b1_ss, b1_rs, 1)
    back_x = Channel(lambda k: [
        (remote(b2_s.at[k % 2, :, block(behind[i])], b2_r.at[k, :, block(behind[i])],
                b2_ss.at[k % 2, i], b2_rs.at[k, i], token=near[2]), has_behind[i], has_ahead[i])
        for i in range(depth - 1)
    ])
    back_z = Channel(lambda k: [
        (remote(b3_s.at[k % 2, i], b3_r.at[k, i], b3_ss.at[k % 2, i], b3_rs.at[k, i],
                neuron=ahead[i]), has_ahead[i], has_behind[i])
        for i in range(depth - 1)
    ])
    back_pair = single(lambda k: b4_s.at[k % 2], lambda k: b4_r.at[k], b4_ss, b4_rs, 2)
    back_t = single(lambda k: bk.at[k, half, :], lambda k: bk.at[k, half, :], b5_ss, b5_rs, 1)

    def product(k):
        @pl.when(k == 0)
        def _():
            load_e.wait()

        hid_core.free(k)
        h_f[...] = jnp.dot(tt[chunk_rows(k), :], e[...], preferred_element_type=f32)
        h_s[k % 2] = h_f[other_half, :]

        @pl.when(k == 0)
        def _():
            load_w.wait()

        lab_core.free(k)

        @pl.loop(0, 2 * cols // TILE)
        def _(n):
            at_w = at(c2 * 2 * cols + n * TILE, TILE, TILE)
            lab_s[k % 2, :, at(n * TILE, TILE, TILE)] = jnp.dot(
                tt[chunk_rows(k), :], w[:, at_w], preferred_element_type=f32
            ).astype(bf16)

        hid_core.start(k)

        @pl.loop(0, 2 * cols // TILE)
        def _(n):
            @pl.when(n == 1)
            def _():
                lab_core.start(k)

            at_w = at(c * 2 * cols + n * TILE, TILE, TILE)
            lab_o[:, at(n * TILE, TILE, TILE)] = jnp.dot(
                tt[chunk_rows(k), :], w[:, at_w], preferred_element_type=f32
            )

        if 2 * cols // TILE < 2:
            lab_core.start(k)

    def label_core(k):
        lab_core.take(k)
        lab_x.free(k)
        there, here = at(x2 * cols, cols, 128), at(x * cols, cols, 128)
        lx_s[k % 2] = (lab_o[:, there] + lab_r[k % 2, :, there].astype(f32)).astype(bf16)
        lab_k[k % KEPT] = lab_o[:, here] + lab_r[k % 2, :, here].astype(f32)

    def hidden_core(k):
        hid_core.take(k)
        hid_x.free(k)
        hx_s[k % 2] = h_f[half, :] + h_r[k]

    def hidden_x(k):
        hid_x.take(k)
        hid_z.free(k)
        hid_block(k, z)[...] = (hx_s[k % 2] + hx_r[k]).astype(bf16)

    def hidden_z(k):
        hid_z.take(k)
        hid_back.free(k)
        hid_kept.free(k)
        hid_back.start(k)
        hid_kept.start(k)

    def hidden_relay(k):
        hid_back.take(k)
        hid_relay.free(k)
        hid_relay.start(k)

    def error(k):
        hid_kept.take(k)
        hid_relay.take(k)

        @pl.when(k == 0)
        def _():
            decoder_own.wait()
            for i in range(1, 4):
                decoder_wait(i)

        lab_x.take(k)
        predicted = jnp.dot(hid[chunk_rows(k), :], dec[...], preferred_element_type=f32)
        labels = jnp.maximum(lab_k[k % KEPT] + lx_r[k % RING].astype(f32), 0.0)
        scaled[chunk_rows(k), :] = ((predicted - labels) * scale).astype(bf16)

    def back_product(k):
        back_core.free(k)
        bo[k % 2] = lax.dot_general(
            scaled[chunk_rows(k), :], dec[...], (((1,), (1,)), ((), ())),
            preferred_element_type=f32,
        )
        b1_s[k % 2] = bo[k % 2, other_half, :].astype(bf16)

    def back_core_sum(k):
        back_core.take(k)
        back_x.free(k)
        total = bo[k % 2, half, :] + b1_r[k].astype(f32)
        bo[k % 2, half, :] = total
        b2_s[k % 2] = total.astype(bf16)

    def back_x_sum(k):
        back_x.take(k)
        back_z.free(k)
        for i in range(depth - 1):
            @pl.when(has_ahead[i])
            def _():
                b3_s[k % 2, i] = (
                    bo[k % 2, half, block(ahead[i])] + b2_r[k, :, block(ahead[i])].astype(f32)
                ).astype(bf16)
        bz[k % 4] = bo[k % 2, half, block(z)]

    def back_z_sum(k):
        back_z.take(k)
        back_pair.free(k)
        for i in range(depth - 1):
            @pl.when(has_behind[i])
            def _():
                bz[k % 4] = bz[k % 4] + b3_r[k, i].astype(f32)
        b4_s[k % 2] = bz[k % 4].astype(bf16)

    def back_pair_sum(k):
        back_pair.take(k)
        back_t.free(k)
        bk[k, half, :] = (bz[k % 4] + b4_r[k].astype(f32)).astype(bf16)

    def encoder_grad(k):
        remote(bk.at[k, other_half, :], bk.at[k, other_half, :],
               b5_ss.at[k % 2], b5_rs.at[k], token=near[1]).wait_recv()
        ge[...] += lax.dot_general(
            bk[k], tt[chunk_rows(k), :], (((0,), (0,)), ((), ())), preferred_element_type=f32
        )

    def far(j):
        fx, fc = 1 - j // 2, (j + j // 2) % 2
        xx = x + fx - 2 * x * fx
        cc = c + fc - 2 * c * fc
        return 2 * xx + cc

    mine = at(quarter[0] * cols, cols, 128)

    def grad_remote(j):
        return remote(gd.at[j], out_d.at[:, mine], gd_ss.at[j], gd_rs.at[j], token=far(j))

    grad_local = pltpu.make_async_copy(gd.at[3], out_d.at[:, mine], gd_ss.at[3])

    def decoder_grad():
        @pl.loop(0, 4)
        def _(j):
            acc[...] = jnp.zeros_like(acc)

            @pl.loop(0, chunks)
            def _(k):
                acc[...] += lax.dot_general(
                    hid[chunk_rows(k), at(far(j) * rank_rows, rank_rows, 128)],
                    scaled[chunk_rows(k), :], (((0,), (0,)), ((), ())), preferred_element_type=f32,
                )
            gd[j] = acc[...].astype(bf16)

            @pl.when(j < 3)
            def _():
                grad_remote(j).start()

            @pl.when(j == 3)
            def _():
                grad_local.start()

    def staged(s, lag, *stages):
        k = s - lag

        @pl.when((k >= 0) & (k < chunks))
        def _():
            for stage in stages:
                stage(k)

    def error_last(k):
        error(k)

        @pl.when(k == chunks - 1)
        def _():
            decoder_grad()

    stages = {
        "product": (product,),
        "label_core": (label_core, lab_x.start),
        "hidden_core": (hidden_core, hid_x.start),
        "hidden_x": (hidden_x, hid_z.start),
        "hidden_z": (hidden_z,),
        "hidden_relay": (hidden_relay,),
        "error": (error_last,),
        "back_product": (back_product, back_core.start),
        "back_core": (back_core_sum, back_x.start),
        "back_x": (back_x_sum, back_z.start),
        "back_z": (back_z_sum, back_pair.start),
        "back_pair": (back_pair_sum, back_t.start),
        "encoder_grad": (encoder_grad,),
    }
    for i in range(4):
        stages[i] = (functools.partial(lambda i, k: forward(k, i), i),)

    @pl.loop(0, chunks + max(lag for _, lag in SCHEDULE))
    def _(s):
        staged(s, -AHEAD, first)
        for name, lag in SCHEDULE:
            staged(s, lag, *stages[name])

    finish = pltpu.make_async_copy(ge, out_e, in_sem.at[0])
    finish.start()

    @pl.when(t != z)
    def _():
        for k in range(chunks):
            first_remote(k).wait_send()

    for i in range(1, 4):
        decoder_copy(i).wait_send()
    for k in range(max(chunks - 2, 0), chunks):
        for i in range(4):
            up_copy, down_copy, goes_up, goes_down = piece(k, i)

            @pl.when(goes_up)
            def _():
                up_copy().wait_send()

            @pl.when(goes_down)
            def _():
                down_copy().wait_send()

    for channel in (lab_core, lab_x, hid_core, hid_x, hid_z, hid_back, hid_kept, hid_relay,
                    back_core, back_x, back_z, back_pair, back_t):
        channel.drain(chunks)
    for j in range(3):
        grad_remote(j).wait_send()
        source = [2, 3, 1][j]
        remote(gd.at[j], out_d.at[:, at(quarter[source] * cols, cols, 128)],
               gd_ss.at[j], gd_rs.at[j], token=near[source]).wait_recv()
    grad_local.wait()
    finish.wait()


def fused(tokens, up_weight, encoder, decoder):
    row_count, width = tokens.shape
    depth = lax.axis_size("neuron")
    block = up_weight.shape[0]
    cols = up_weight.shape[1] // 4
    rank_part = encoder.shape[1]
    rank_rows = decoder.shape[0]
    rank = rank_rows * 4
    g = min(PIECE_ROWS, row_count)
    chunks = row_count // g
    rows = 4 * g
    total = rows * chunks
    scale = 1.0 / math.sqrt(total)
    sizes = (chunks, g, width, cols, rank_part, rank_rows, depth, scale)
    f32, bf16 = jnp.float32, jnp.bfloat16
    vmem = pltpu.VMEM
    dma = pltpu.SemaphoreType.DMA
    scratch = [
        vmem((block, 4 * cols), bf16), vmem((block, rank_part), bf16), vmem((total, block), bf16),
        vmem((rank, cols), bf16), vmem((total, rank), bf16), vmem((total, cols), bf16),
        vmem((2, rows, 2 * cols), bf16), vmem((2, rows, 2 * cols), bf16),
        vmem((rows, 2 * cols), f32), vmem((KEPT, rows, cols), f32),
        vmem((2, rows, cols), bf16), vmem((RING, rows, cols), bf16),
        vmem((2, 2 * g, rank_part), f32), vmem((rows, rank_part), f32),
        vmem((chunks, 2 * g, rank_part), f32),
        vmem((2, 2 * g, rank_part), f32), vmem((chunks, 2 * g, rank_part), f32),
        vmem((2, rows, rank), f32), vmem((2, 2 * g, rank), bf16), vmem((chunks, 2 * g, rank), bf16),
        vmem((2, 2 * g, rank), bf16), vmem((chunks, 2 * g, rank), bf16),
        vmem((2, depth - 1, 2 * g, rank_part), bf16),
        vmem((chunks, depth - 1, 2 * g, rank_part), bf16),
        vmem((2, 2 * g, rank_part), bf16), vmem((chunks, 2 * g, rank_part), bf16),
        vmem((4, 2 * g, rank_part), f32), vmem((chunks, rows, rank_part), bf16),
        vmem((rank_part, block), f32), vmem((4, rank_rows, cols), bf16), vmem((rank_rows, cols), f32),
        dma((2,)), dma((chunks, 4)), dma((chunks,)), dma((2, 4, 2)), dma((4,)), dma((4,)),
        dma((2,)), dma((2,)), dma((2,)), dma((chunks,)),
        dma((2,)), dma((chunks,)), dma((2,)), dma((chunks,)),
        dma((2, depth - 1)), dma((chunks, depth - 1)), dma((2, depth - 1)), dma((chunks, depth - 1)),
        dma((2, depth)), dma((chunks, depth)), dma((2, depth - 1)), dma((chunks, depth - 1)),
        dma((2,)), dma((chunks,)), dma((2, depth - 1)), dma((chunks, depth - 1)),
        dma((2, depth - 1)), dma((chunks, depth - 1)), dma((2,)), dma((chunks,)),
        dma((2,)), dma((chunks,)), dma((4,)), dma((4,)),
    ]
    anywhere = pl.BlockSpec(memory_space=pl.ANY)
    grad_e, grad_d = pl.pallas_call(
        functools.partial(step_kernel, sizes),
        out_shape=(
            jax.ShapeDtypeStruct((rank_part, block), f32),
            jax.ShapeDtypeStruct((rank_rows, 4 * cols), bf16),
        ),
        in_specs=[anywhere] * 4,
        out_specs=(anywhere, anywhere),
        scratch_shapes=scratch,
        compiler_params=pltpu.CompilerParams(
            collective_id=0, has_side_effects=True, vmem_limit_bytes=VMEM_BYTES
        ),
        name="step",
    )(tokens, up_weight, encoder, decoder)
    return grad_e.T, grad_d.astype(f32)


def fits(mesh, tokens, up_weight, encoder, decoder):
    deep, wide = mesh.shape["neuron"], mesh.shape["token"]
    row_count = tokens.shape[0] // (mesh.shape["layer"] * wide)
    return (
        wide == 4
        and deep == wide
        and up_weight.shape[1] % (deep * wide * 128) == 0
        and up_weight.shape[1] % (deep * 2 * TILE) == 0
        and encoder.shape[1] % (deep * 128) == 0
        and row_count % PIECE_ROWS == 0
    )


def multiply(left, right):
    return jnp.dot(left, right, preferred_element_type=jnp.float32)


def contract_rows(left, right):
    return lax.dot_general(
        left, right, (((0,), (0,)), ((), ())), preferred_element_type=jnp.float32
    )


def swap(value, axis, offset):
    size = lax.axis_size(axis)
    return lax.ppermute(value, axis, [(i, i ^ offset) for i in range(size)])


def block_at(value, index, width, dim):
    return lax.dynamic_slice_in_dim(value, index * width, width, dim)


def after(value, *earlier):
    return lax.optimization_barrier((value, *earlier))[0]


def reduce_relative(terms_of, axis, wire, trace=None):
    size = lax.axis_size(axis)
    ks = list(range(size))
    held = None
    bit = 1
    while bit < size:
        kept = [k for k in ks if not k & bit]
        sent = [k for k in ks if k & bit]
        if held is None:
            outgoing = terms_of(sent).astype(wire)
            own = terms_of(kept) if trace is None else terms_of(kept, outgoing)
        else:
            outgoing = jnp.stack([held[ks.index(k)] for k in sent]).astype(wire)
            own = jnp.stack([held[ks.index(k)] for k in kept])
        if trace is not None:
            trace.append([outgoing, own])
        held = own + swap(outgoing, axis, bit).astype(jnp.float32)
        ks = kept
        bit *= 2
    if held is None:
        held = terms_of(ks)
    return held[0]


def gather_absolute(value, axis):
    size = lax.axis_size(axis)
    me = lax.axis_index(axis)
    held = value[None]
    order = [0]
    bit = size // 2
    while bit:
        held = jnp.concatenate([held, swap(held, axis, bit)])
        order = order + [k ^ bit for k in order]
        bit //= 2
    place = [order.index(k) for k in range(size)]
    relative = [held[p] for p in place]
    for level in range(size.bit_length() - 1):
        step = 1 << level
        flip = (me & step) != 0
        relative = [
            jnp.where(flip, relative[j ^ step], relative[j]) for j in range(size)
        ]
    return jnp.concatenate(relative)


def per_device(tokens, up_weight, encoder, decoder):
    token_size = lax.axis_size("token")
    neuron_size = lax.axis_size("neuron")
    t = lax.axis_index("token")
    n = lax.axis_index("neuron")
    row_count, width = tokens.shape
    rank_part = encoder.shape[1]
    rank = decoder.shape[0] * token_size
    rank_rows = decoder.shape[0]
    features = width * neuron_size // token_size
    blocks = neuron_size // token_size
    total_rows = row_count * token_size
    chunks = CHUNKS
    rows = row_count // chunks
    scale = 1.0 / math.sqrt(total_rows)

    gathered = [
        lax.all_gather(tokens[c * rows : (c + 1) * rows], "neuron", axis=0, tiled=False)
        for c in range(chunks)
    ]
    decoder_whole = gather_absolute(decoder, "token")

    hiddens, errors, all_pieces = [], [], []
    previous, gates = None, []
    for c in range(chunks):
        source = gathered[c] if previous is None else after(gathered[c], *gates[-1])
        grouped = source.reshape(token_size, blocks, rows, width)

        def features_for(k):
            mine = lax.dynamic_index_in_dim(grouped, t ^ k, 0, keepdims=False)
            return mine.transpose(1, 0, 2).reshape(rows, features)

        pieces = [features_for(0)] + [
            swap(features_for(k), "token", k) for k in range(1, token_size)
        ]
        if previous is not None:
            pieces[1] = after(pieces[1], *previous)

        def terms(ks, weight, earlier=None):
            left = jnp.concatenate([pieces[k] for k in ks])
            if earlier is not None:
                left = after(left, earlier)
            return multiply(left, weight).reshape(len(ks), rows, weight.shape[1])

        label_trace = []
        sums = reduce_relative(
            lambda ks, earlier=None: terms(ks, up_weight, earlier),
            "token",
            jnp.bfloat16,
            label_trace,
        )
        hidden_part = reduce_relative(
            lambda ks: terms(ks, encoder), "token", jnp.float32
        ).astype(jnp.bfloat16)
        others = jnp.stack(
            [hidden_part]
            + [swap(hidden_part, "neuron", m) for m in range(1, neuron_size)]
        )
        hidden = jnp.concatenate(
            [
                lax.dynamic_index_in_dim(others, n ^ j, 0, keepdims=False)
                for j in range(neuron_size)
            ],
            axis=1,
        )
        labels = jax.nn.relu(sums)
        predicted = multiply(hidden, decoder_whole)
        scaled = ((predicted - labels) * scale).astype(jnp.bfloat16)
        previous = label_trace[-1][:1] + errors[-1:]
        gates.append(label_trace[0])
        hiddens.append(hidden)
        errors.append(scaled)
        all_pieces.append(pieces)

    hidden = jnp.concatenate(hiddens)
    scaled = jnp.concatenate(errors)
    columns = scaled.shape[1] // COLUMN_PARTS
    relative = [block_at(hidden, t ^ k, rank_rows, 1) for k in range(token_size)]
    grads = []
    for p in range(COLUMN_PARTS):
        part = scaled[:, p * columns : (p + 1) * columns]

        def grad_terms(ks, part=part):
            left = jnp.concatenate([relative[k] for k in ks], axis=1)
            return contract_rows(left, part).reshape(len(ks), rank_rows, columns)

        grads.append(reduce_relative(grad_terms, "token", jnp.bfloat16))

    back_terms = lax.dot_general(
        scaled, decoder_whole, (((1,), (1,)), ((), ())), preferred_element_type=jnp.float32
    )
    back = block_at(back_terms, n, rank_part, 1)
    for m in range(1, neuron_size):
        outgoing = block_at(back_terms, n ^ m, rank_part, 1).astype(jnp.bfloat16)
        back = back + swap(outgoing, "neuron", m).astype(jnp.float32)
    back = back.astype(jnp.bfloat16)
    backs = [back] + [swap(back, "token", k) for k in range(1, token_size)]
    grad_encoder = contract_rows(
        jnp.concatenate([pieces[k] for k in range(token_size) for pieces in all_pieces]),
        jnp.concatenate(backs),
    )
    return (grad_encoder, jnp.concatenate(grads, axis=1))


def solution(mesh):
    spec = P(("layer", "token"), "neuron")

    def step(tokens, up_weight, encoder, decoder):
        local = fused if fits(mesh, tokens, up_weight, encoder, decoder) else per_device
        return jax.shard_map(
            local, mesh=mesh, in_specs=(spec,) * 4, out_specs=(spec, spec), check_vma=False
        )(tokens, up_weight, encoder, decoder)

    return step
```
